32 devices in a mesh: smp: 8 (over z, y), var: 4 (over x, core).
Axes of the slice: x: 2, y: 2, z: 4, core: 2. Of those that a mesh axis runs over, the one named last changes fastest.
Arguments:
- dosage: int32 [512, 2048], P('smp', 'var'), may hold values from -2147483648 to 2147483647, as said below
- shares_init: float32 [12, 8192], P(None, ('smp', 'var')), may hold values from 0.1 to 1
- freqs_init: float32 [12, 2048], P(None, ('var', 'smp')), may hold values from 0.019 to 0.981
Outputs:
- shares: float32 [12, 8192], P(None, ('smp', 'var'))
- freqs: float32 [12, 2048], P(None, ('var', 'smp'))
The draws below stay inside these ranges and needn't reach their ends.
Inputs may be any that keep to these rules, and one draw needn't show every extreme that they name: Every 2-bit code in a word of dosage is 0, 1, 2 or 3, and 3 marks a missing genotype.
All inputs are finite; a program needn't handle non-finite values.
Results may differ from the reference program's by a relative error of at most 0.0003.
Values sent between devices are 32-bit elements; how exact they have to be, the bound alone decides.
A program may use at most 64 MiB of HBM per device.

```python
import math
import jax
import jax.numpy as jnp
from jax import lax

K = 12
ITERS = 2
R_DEV = 1024
N = 8192
M = 2048


def planted_weights(key):
    weight_key = jax.random.fold_in(key, 201)
    cube_base = jax.random.randint(jax.random.fold_in(weight_key, 1), (K, N), 0, 16, dtype=jnp.int32)
    leading = jax.random.randint(jax.random.fold_in(weight_key, 2), (N,), 0, K, dtype=jnp.int32)
    boost = jnp.where(jnp.arange(K, dtype=jnp.int32)[:, None] == leading[None, :], 20000, 0)
    return cube_base * cube_base * cube_base + 1 + boost


def planted_levels(key):
    level_key = jax.random.fold_in(key, 202)
    spread = jax.random.randint(jax.random.fold_in(level_key, 1), (K, M), 0, 992, dtype=jnp.int32)
    flipped = jax.random.randint(jax.random.fold_in(level_key, 2), (K, M), 0, 2, dtype=jnp.int32)
    lower = 16 + spread * spread // 992
    return jnp.where(flipped == 1, 1024 - lower, lower)


def draw_dosage(key, part):
    weights = planted_weights(key)
    levels = planted_levels(key)
    grouped = weights.reshape(K, N // 16, 16)
    genotype_key = jax.random.fold_in(key, 203)

    def add_codes(position, packed):
        picked = lax.dynamic_index_in_dim(grouped, position, 2, keepdims=False)
        numerator = jnp.dot(picked.T, levels)
        denominator = jnp.sum(picked, axis=0) * 1024
        sample_key = jax.random.fold_in(genotype_key, position)
        limit = jnp.broadcast_to(denominator[:, None], numerator.shape)
        first_draw = jax.random.randint(jax.random.fold_in(sample_key, 1), numerator.shape, 0, limit, dtype=jnp.int32)
        second_draw = jax.random.randint(jax.random.fold_in(sample_key, 2), numerator.shape, 0, limit, dtype=jnp.int32)
        alleles = (first_draw < numerator).astype(jnp.int32) + (second_draw < numerator).astype(jnp.int32)
        absent = jax.random.randint(jax.random.fold_in(sample_key, 3), numerator.shape, 0, 10, dtype=jnp.int32) == 0
        codes = jnp.where(absent, 3, alleles)
        return jnp.bitwise_or(packed, jnp.left_shift(codes, 2 * position))
    return lax.fori_loop(0, 16, add_codes, jnp.zeros((N // 16, M), jnp.int32))


def draw_freqs_init(key, part):
    levels = planted_levels(key)
    base = levels.astype(jnp.float32) / 1024.0
    noise = jax.random.uniform(jax.random.fold_in(key, 204), (K, M), jnp.float32, 0.05, 0.95)
    return 0.9 * base + 0.1 * noise


def shard_levels(stream_key, dims, cuts, least, high):
    def one(dim, parts):
        heights = jax.random.uniform(jax.random.fold_in(jax.random.fold_in(stream_key, 6), dim), (parts,), jnp.float32, least / len(cuts), high / len(cuts))
        return jnp.repeat(jnp.exp(heights), dims[dim] // parts).reshape((-1,) + (1,) * (len(dims) - dim - 1))

    loudness = one(*cuts[0])
    for cut in cuts[1:]:
        loudness = loudness * one(*cut)
    return loudness


def setup_inputs(seed: int = 0) -> dict:
    key_list = jax.random.split(jax.random.key(seed), 4)
    dosage = draw_dosage(jax.random.fold_in(key_list[3], 71), 0)
    shares_init = jnp.clip(jnp.exp(math.log(1.0) - 2.3025851 * jax.random.uniform(key_list[1], (K, N), jnp.float32) ** shard_levels(key_list[1], (K, N), ((1, 32),), -0.2, 0.2)), 0.1, 1.0)
    freqs_init = draw_freqs_init(jax.random.fold_in(key_list[3], 71), 0)
    return dict(dosage=dosage, shares_init=shares_init, freqs_init=freqs_init)


HIGH = lax.Precision.HIGHEST


def unpack_codes(packed):
    shifts = 2 * jnp.arange(16, dtype=jnp.int32)
    codes = jnp.bitwise_and(jnp.right_shift(packed[:, None, :], shifts[None, :, None]), 3)
    return codes.reshape(packed.shape[0] * 16, packed.shape[1])


def expect_sums(packed, shares_block, freqs_block):
    codes = unpack_codes(packed)
    live = (codes < 3).astype(jnp.float32)
    allele_f = live * codes.astype(jnp.float32)
    probs = jnp.einsum("kn,km->nm", shares_block, freqs_block, precision=HIGH)
    ratio_alt = allele_f / probs
    ratio_ref = (2.0 * live - allele_f) / (1.0 - probs)
    sum_q = jnp.einsum("km,nm->kn", freqs_block, ratio_alt, precision=HIGH) + jnp.einsum("km,nm->kn", 1.0 - freqs_block, ratio_ref, precision=HIGH)
    sum_a = jnp.einsum("kn,nm->km", shares_block, ratio_alt, precision=HIGH)
    sum_b = jnp.einsum("kn,nm->km", shares_block, ratio_ref, precision=HIGH)
    return sum_q, sum_a, sum_b


def renew_shares(shares_block, sum_q):
    numer = shares_block * sum_q
    return (numer + 0.5) / (jnp.sum(numer, axis=0, keepdims=True) + 0.5 * shares_block.shape[0])


def renew_freqs(freqs_block, sum_a, sum_b):
    alt_part = freqs_block * sum_a
    ref_part = (1.0 - freqs_block) * sum_b
    return (alt_part + 0.5) / (alt_part + ref_part + 1.0)


def reference(dosage, shares_init, freqs_init):
    shares_now = shares_init / jnp.sum(shares_init, axis=0, keepdims=True)
    freqs_now = freqs_init
    blocks = dosage.shape[0] * 16 // R_DEV
    packed_blocks = dosage.reshape(blocks, R_DEV // 16, dosage.shape[1])
    for iteration in range(ITERS):
        share_blocks = shares_now.reshape(K, blocks, R_DEV).transpose(1, 0, 2)

        def one_block(carry, items):
            sum_q, sum_a, sum_b = expect_sums(items[0], items[1], freqs_now)
            return (carry[0] + sum_a, carry[1] + sum_b), sum_q

        start = (jnp.zeros(freqs_now.shape, jnp.float32), jnp.zeros(freqs_now.shape, jnp.float32))
        totals, sums_q = lax.scan(one_block, start, (packed_blocks, share_blocks))
        sum_q = sums_q.transpose(1, 0, 2).reshape(K, shares_now.shape[1])
        new_shares = renew_shares(shares_now, sum_q)
        freqs_now = renew_freqs(freqs_now, totals[0], totals[1])
        shares_now = new_shares
    return shares_now, freqs_now
```

```python
import functools

import jax
import jax.numpy as jnp
from jax import lax
from jax.experimental import pallas as pl
from jax.experimental.pallas import tpu as pltpu
from jax.sharding import PartitionSpec as P

ITERS = 2
CODES = 16
PAD = 16
ROWS = 512
F32 = jnp.float32
BF16 = jnp.bfloat16


def split(x, pieces):
    out = []
    for _ in range(pieces):
        piece = x.astype(BF16)
        out.append(piece)
        x = x - piece.astype(F32)
    return out


def dot(a, b):
    return jnp.dot(a, b, preferred_element_type=F32)


def dot_nt(a, b):
    return lax.dot_general(a, b, (((1,), (1,)), ((), ())), preferred_element_type=F32)


def em_kernel(
    nv, ns, dosage_hbm, shares_hbm, freqs_hbm, shares_out, freqs_out,
    dosage_ref, shares_ref, freqs_ref, alt_ref, ref_ref,
    q_slots, f_slots, c_slots, sq_send, sq_recv, sc_send, sc_recv, sf_send, sf_recv,
    q_pad, f_pad, qt_ref, qd_ref, qb_ref, fs_ref, fgs_ref,
    load_sem, q_ss, q_rs, f_ss, f_rs, c_ss, c_rs, sq_ss, sq_rs, sc_ss, sc_rs, sf_ss, sf_rs,
):
    iv, js = lax.axis_index("var"), lax.axis_index("smp")
    pops, ws = shares_ref.shape
    wf = freqs_ref.shape[1]
    words, variants = dosage_ref.shape
    samples = words * CODES
    half = ns // 2
    mids = half // 2
    chunk = variants // 2
    wc = chunk // mids
    side = js // half
    mesh_ids = pl.DeviceIdType.MESH

    def other_smp(d):
        return lax.rem(js + d, ns)

    def middle(c, i):
        return (1 - c) * half + c * (half - mids) + i

    my_mid_chunk = 1 - side
    my_mid = js - middle(my_mid_chunk, 0)
    is_mid = jnp.logical_and(js >= half - mids, js < half + mids)
    smp_peers = [other_smp(d) for d in range(1, ns)]
    var_peers = [lax.rem(iv + d, nv) for d in range(1, nv)]

    barrier = pltpu.get_barrier_semaphore()
    for p in smp_peers:
        pl.semaphore_signal(barrier, inc=1, device_id=(p, iv), device_id_type=mesh_ids)
    for p in var_peers:
        pl.semaphore_signal(barrier, inc=1, device_id=(js, p), device_id_type=mesh_ids)

    load_q = pltpu.make_async_copy(shares_hbm, shares_ref, load_sem.at[0])
    load_f = pltpu.make_async_copy(freqs_hbm, f_slots.at[js], load_sem.at[1])
    load_d = pltpu.make_async_copy(dosage_hbm, dosage_ref, load_sem.at[2])
    load_q.start()
    load_f.start()
    load_d.start()
    q_pad[...] = jnp.zeros_like(q_pad)
    f_pad[...] = jnp.zeros_like(f_pad)
    load_q.wait()
    q_own = shares_ref[...]
    q_own = q_own / jnp.sum(q_own, axis=0, keepdims=True)
    q_slots[0, iv] = q_own
    load_f.wait()
    pl.semaphore_wait(barrier, ns - 1 + nv - 1)

    def smp_copy(src, dst, ss, rs, to):
        return pltpu.make_async_remote_copy(
            src_ref=src, dst_ref=dst, send_sem=ss, recv_sem=rs, device_id=(to, iv), device_id_type=mesh_ids)

    def var_copy(src, dst, ss, rs, to):
        return pltpu.make_async_remote_copy(
            src_ref=src, dst_ref=dst, send_sem=ss, recv_sem=rs, device_id=(js, to), device_id_type=mesh_ids)

    def f_copy(to, slot):
        return smp_copy(f_slots.at[slot], f_slots.at[slot], f_ss.at[to], f_rs.at[slot], to)

    def q_copy(it, to, slot):
        return var_copy(q_slots.at[it, slot], q_slots.at[it, slot], q_ss.at[it, to], q_rs.at[it, slot], to)

    def sq_copy(it, to, slot):
        return var_copy(sq_send.at[it, to], sq_recv.at[it, slot], sq_ss.at[it, to], sq_rs.at[it, slot], to)

    def sf_copy(to, slot):
        return smp_copy(sf_send.at[to], sf_recv.at[slot], sf_ss.at[to], sf_rs.at[slot], to)

    def sc_copy(it, c, i, to, slot):
        return smp_copy(sc_send.at[it, c, i], sc_recv.at[it, slot], sc_ss.at[it, c, i], sc_rs.at[it, slot], to)

    def c_copy(it, to, slot):
        return smp_copy(c_slots.at[it, slot], c_slots.at[it, slot], c_ss.at[it, to], c_rs.at[it, slot], to)

    sent = []

    def start(copy, when=None):
        sent.append((copy, when))
        if when is None:
            copy.start()
        else:
            pl.when(when)(copy.start)

    for p in smp_peers:
        start(f_copy(p, js))
    for p in var_peers:
        start(q_copy(0, p, iv))

    load_d.wait()
    blocks = samples // ROWS
    ones = jnp.ones((8, chunk), BF16)
    counts = []
    for b in range(blocks):
        here = slice(b * ROWS, (b + 1) * ROWS)
        count = jnp.zeros((8, ROWS), F32)
        for c in range(2):
            packed = dosage_ref[b * ROWS // CODES:(b + 1) * ROWS // CODES, c * chunk:(c + 1) * chunk]
            shape3 = (ROWS // CODES, CODES, chunk)
            shifts = 2 * lax.broadcasted_iota(jnp.int32, shape3, 1)
            codes = jnp.bitwise_and(jnp.right_shift(jnp.broadcast_to(packed[:, None, :], shape3), shifts), 3)
            codes = codes.reshape(ROWS, chunk)
            live = codes < 3
            alt = jnp.where(live, codes.astype(F32), 0.0)
            both = jnp.where(live, 2.0, 0.0)
            alt_ref[c, here, :] = alt
            ref_ref[c, here, :] = both - alt
            count = count + dot_nt(ones, both.astype(BF16))
        counts.append(count[0:1])
    counts = jnp.concatenate(counts, axis=1)

    for it in range(ITERS):
        last = it + 1 == ITERS

        for p in var_peers:
            q_copy(it, p, p).wait_recv()
        for v in range(nv):
            q_pad[0:pops, v * ws:(v + 1) * ws] = q_slots[it, v]
        qh, qm, ql = split(q_pad[...], 3)
        qs = jnp.concatenate([qh, qh, qm, qh, qm, ql, qm, ql], axis=0)
        qt_ref[...] = qs.astype(F32).T.astype(BF16)
        none = jnp.zeros_like(qh)
        qd_ref[...] = jnp.concatenate([qh, none, qm, none], axis=0)
        qb_ref[...] = jnp.concatenate([none, qh, none, qm], axis=0)

        sq_acc = [jnp.zeros((2 * PAD, ROWS), F32) for _ in range(blocks)]
        for t in range(2):
            c = side if (it == 0) == (t == 0) else 1 - side
            if it == 0:
                for i in range(half):
                    p = c * half + lax.rem(js + i, half)
                    if t or i:
                        f_copy(p, p).wait_recv()
                for i in range(half):
                    f_pad[0:pops, i * wf:(i + 1) * wf] = f_slots[c * half + i]
            else:
                for i in range(mids):
                    slot = c * mids + i
                    copy = c_copy(it, js, slot)
                    pl.when(middle(c, i) != js)(copy.wait_recv)
                for i in range(mids):
                    f_pad[0:pops, i * wc:(i + 1) * wc] = c_slots[it, c * mids + i]
            f_all = f_pad[...]
            fh, fm, fl = split(f_all, 3)
            fs_ref[...] = jnp.concatenate([fh, fm, fh, fl, fm, fh, fl, fm], axis=0)
            fpair = jnp.concatenate([fh, fm], axis=0)
            fgs_ref[...] = jnp.concatenate([fpair, fpair], axis=1)

            kept = []
            sums = jnp.zeros((4 * PAD, chunk), F32)
            for b in range(blocks):
                here = slice(b * ROWS, (b + 1) * ROWS)
                probs = dot(qt_ref[here, :], fs_ref[...])
                rest = 1.0 - probs
                inv = 1.0 / (probs * rest)
                alt = alt_ref[c, here, :] * rest
                bb = ref_ref[c, here, :] * probs
                dd = (alt - bb) * inv
                bb = bb * inv
                dh, dl = split(dd, 2)
                bh, bl = split(bb, 2)
                qd, qb = qd_ref[:, here], qb_ref[:, here]
                sums = sums + dot(
                    jnp.concatenate([qd, qd, qb, qb], axis=1), jnp.concatenate([dh, dl, bh, bl], axis=0))
                kept.append(jnp.concatenate([dh, dl], axis=1))
                if t == 0:
                    sq_acc[b] = sq_acc[b] + dot_nt(fgs_ref[...], kept[b])
            sums = sums[0:2 * PAD] + sums[2 * PAD:4 * PAD]
            sum_d, sum_b = sums[0:pops], sums[PAD:PAD + pops]
            if last:
                for i in range(half):
                    cut = slice(i * wf, (i + 1) * wf)
                    sf_send[c * half + i] = jnp.concatenate([sum_d[:, cut], sum_b[:, cut]], axis=1)
                for i in range(half):
                    p = c * half + lax.rem(js + i, half)
                    if i or t == 0:
                        start(sf_copy(p, js))
            else:
                stacked = jnp.concatenate([sum_d, sum_b], axis=0)
                for i in range(mids):
                    sc_send[it, c, i] = stacked[:, i * wc:(i + 1) * wc]
                for i in range(mids):
                    to = middle(c, i)
                    start(sc_copy(it, c, i, to, js), to != js)

        for b in range(blocks):
            sq_acc[b] = sq_acc[b] + dot_nt(fgs_ref[...], kept[b])
        sum_q = jnp.concatenate([x[0:PAD] + x[PAD:2 * PAD] for x in sq_acc], axis=1)
        sum_q = sum_q + (counts - jnp.sum(q_pad[...] * sum_q, axis=0, keepdims=True))
        sum_q = sum_q[0:pops]
        for v in range(nv):
            sq_send[it, v] = sum_q[:, v * ws:(v + 1) * ws]
        for p in var_peers:
            start(sq_copy(it, p, iv))

        total = sq_send[it, iv]
        for p in var_peers:
            sq_copy(it, p, p).wait_recv()
            total = total + sq_recv[it, p]
        numer = q_own * total
        q_own = (numer + 0.5) / (jnp.sum(numer, axis=0, keepdims=True) + 0.5 * pops)
        if last:
            shares_out[...] = q_own
        else:
            q_slots[it + 1, iv] = q_own
            for p in var_peers:
                start(q_copy(it + 1, p, iv))

        if last:
            place = lax.rem(js, half)
            pair = c_slots[it, side * mids + place // 2]
            f_own = jnp.where(lax.rem(place, 2) == 0, pair[:, 0:wf], pair[:, wf:2 * wf])
            total = sf_send[js]
            for p in smp_peers:
                sf_copy(p, p).wait_recv()
                total = total + sf_recv[p]
            sum_d, sum_b = total[:, 0:wf], total[:, wf:2 * wf]
            freqs_out[...] = (f_own * (sum_d + sum_b) + 0.5) / (f_own * sum_d + sum_b + 1.0)
        else:
            slot = my_mid_chunk * mids + my_mid

            @pl.when(is_mid)
            def _():
                total = sc_send[it, my_mid_chunk, my_mid]
                for p in smp_peers:
                    sc_copy(it, my_mid_chunk, my_mid, js, p).wait_recv()
                    total = total + sc_recv[it, p]
                if it == 0:
                    first = my_mid_chunk * half + 2 * my_mid
                    f_old = jnp.concatenate([f_slots[first], f_slots[first + 1]], axis=1)
                else:
                    f_old = c_slots[it, slot]
                sum_d, sum_b = total[0:pops], total[pops:2 * pops]
                c_slots[it + 1, slot] = (f_old * (sum_d + sum_b) + 0.5) / (f_old * sum_d + sum_b + 1.0)

            for p in smp_peers:
                start(c_copy(it + 1, p, slot), is_mid)

    for copy, when in sent:
        if when is None:
            copy.wait_send()
        else:
            pl.when(when)(copy.wait_send)


def hand_out(shares_ref, freqs_ref, shares_out, freqs_out):
    shares_out[...] = shares_ref[...]
    freqs_out[...] = freqs_ref[...]


def body(nv, ns, dosage, shares_init, freqs_init):
    pops, ws = shares_init.shape
    wf = freqs_init.shape[1]
    words, variants = dosage.shape
    samples = words * CODES
    chunk = variants // 2
    mids = ns // 4
    wc = chunk // mids
    vmem = pl.BlockSpec(memory_space=pltpu.VMEM)
    hbm = pl.BlockSpec(memory_space=pl.ANY)
    dma = pltpu.SemaphoreType.DMA
    shapes = (jax.ShapeDtypeStruct((pops, ws), F32), jax.ShapeDtypeStruct((pops, wf), F32))
    shares, freqs = pl.pallas_call(
        functools.partial(em_kernel, nv, ns),
        out_shape=shapes,
        in_specs=[hbm, hbm, hbm],
        out_specs=(vmem, vmem),
        scratch_shapes=[
            pltpu.VMEM((words, variants), jnp.int32),
            pltpu.VMEM((pops, ws), F32),
            pltpu.VMEM((pops, wf), F32),
            pltpu.VMEM((2, samples, chunk), F32),
            pltpu.VMEM((2, samples, chunk), F32),
            pltpu.VMEM((ITERS, nv, pops, ws), F32),
            pltpu.VMEM((ns, pops, wf), F32),
            pltpu.VMEM((ITERS, 2 * mids, pops, wc), F32),
            pltpu.VMEM((ITERS, nv, pops, ws), F32),
            pltpu.VMEM((ITERS, nv, pops, ws), F32),
            pltpu.VMEM((ITERS, 2, mids, 2 * pops, wc), F32),
            pltpu.VMEM((ITERS, ns, 2 * pops, wc), F32),
            pltpu.VMEM((ns, pops, 2 * wf), F32),
            pltpu.VMEM((ns, pops, 2 * wf), F32),
            pltpu.VMEM((PAD, samples), F32),
            pltpu.VMEM((PAD, chunk), F32),
            pltpu.VMEM((samples, 8 * PAD), BF16),
            pltpu.VMEM((4 * PAD, samples), BF16),
            pltpu.VMEM((4 * PAD, samples), BF16),
            pltpu.VMEM((8 * PAD, chunk), BF16),
            pltpu.VMEM((2 * PAD, 2 * chunk), BF16),
            dma((3,)),
            dma((ITERS, nv)), dma((ITERS, nv)),
            dma((ns,)), dma((ns,)),
            dma((ITERS, ns)), dma((ITERS, 2 * mids)),
            dma((ITERS, nv)), dma((ITERS, nv)),
            dma((ITERS, 2, mids)), dma((ITERS, ns)),
            dma((ns,)), dma((ns,)),
        ],
        compiler_params=pltpu.CompilerParams(collective_id=0, has_side_effects=True),
        cost_estimate=pl.CostEstimate(flops=200000000, bytes_accessed=400000, transcendentals=1000000),
    )(dosage, shares_init, freqs_init)
    return pl.pallas_call(
        hand_out, out_shape=shapes, in_specs=[vmem, vmem], out_specs=(vmem, vmem),
    )(shares, freqs)


def solution(mesh):
    placed = (P("smp", "var"), P(None, ("smp", "var")), P(None, ("var", "smp")))
    return jax.shard_map(
        functools.partial(body, mesh.shape["var"], mesh.shape["smp"]),
        mesh=mesh,
        in_specs=placed,
        out_specs=(P(None, ("smp", "var")), P(None, ("var", "smp"))),
        check_vma=False,
    )
```

```python
import functools

import jax
import jax.numpy as jnp
from jax import lax
from jax.experimental import pallas as pl
from jax.experimental.pallas import tpu as pltpu
from jax.sharding import PartitionSpec as P

ITERS = 2
CODES = 16
PAD = 16
ROWS = 512
F32 = jnp.float32
BF16 = jnp.bfloat16


def split(x, pieces):
    out = []
    for _ in range(pieces):
        piece = x.astype(BF16)
        out.append(piece)
        x = x - piece.astype(F32)
    return out


def dot(a, b):
    return jnp.dot(a, b, preferred_element_type=F32)


def dot_nt(a, b):
    return lax.dot_general(a, b, (((1,), (1,)), ((), ())), preferred_element_type=F32)


def em_kernel(
    nv, ns, dosage_hbm, shares_hbm, freqs_hbm, shares_out, freqs_out,
    dosage_ref, shares_ref, freqs_ref, alt_ref, ref_ref,
    q_slots, f_slots, c_slots, sq_send, sq_recv, sc_send, sc_recv, sf_send, sf_recv,
    q_pad, f_pad, qt_ref, qd_ref, qb_ref, fs_ref, fgs_ref,
    load_sem, q_ss, q_rs, f_ss, f_rs, c_ss, c_rs, sq_ss, sq_rs, sc_ss, sc_rs, sf_ss, sf_rs,
):
    iv, js = lax.axis_index("var"), lax.axis_index("smp")
    pops, ws = shares_ref.shape
    wf = freqs_ref.shape[1]
    words, variants = dosage_ref.shape
    samples = words * CODES
    half = ns // 2
    mids = half // 2
    chunk = variants // 2
    wc = chunk // mids
    side = js // half
    mesh_ids = pl.DeviceIdType.MESH

    def other_smp(d):
        return lax.rem(js + d, ns)

    def middle(c, i):
        return (1 - c) * half + c * (half - mids) + i

    my_mid_chunk = 1 - side
    my_mid = js - middle(my_mid_chunk, 0)
    is_mid = jnp.logical_and(js >= half - mids, js < half + mids)
    smp_peers = [other_smp(d) for d in range(1, ns)]
    var_peers = [lax.rem(iv + d, nv) for d in range(1, nv)]

    barrier = pltpu.get_barrier_semaphore()
    for p in smp_peers:
        pl.semaphore_signal(barrier, inc=1, device_id=(p, iv), device_id_type=mesh_ids)
    for p in var_peers:
        pl.semaphore_signal(barrier, inc=1, device_id=(js, p), device_id_type=mesh_ids)

    load_q = pltpu.make_async_copy(shares_hbm, shares_ref, load_sem.at[0])
    load_f = pltpu.make_async_copy(freqs_hbm, f_slots.at[js], load_sem.at[1])
    load_d = pltpu.make_async_copy(dosage_hbm, dosage_ref, load_sem.at[2])
    load_q.start()
    load_f.start()
    load_d.start()
    q_pad[...] = jnp.zeros_like(q_pad)
    f_pad[...] = jnp.zeros_like(f_pad)
    load_q.wait()
    q_own = shares_ref[...]
    q_own = q_own / jnp.sum(q_own, axis=0, keepdims=True)
    q_slots[0, iv] = q_own
    load_f.wait()
    pl.semaphore_wait(barrier, ns - 1 + nv - 1)

    def smp_copy(src, dst, ss, rs, to):
        return pltpu.make_async_remote_copy(
            src_ref=src, dst_ref=dst, send_sem=ss, recv_sem=rs, device_id=(to, iv), device_id_type=mesh_ids)

    def var_copy(src, dst, ss, rs, to):
        return pltpu.make_async_remote_copy(
            src_ref=src, dst_ref=dst, send_sem=ss, recv_sem=rs, device_id=(js, to), device_id_type=mesh_ids)

    def f_copy(to, slot):
        return smp_copy(f_slots.at[slot], f_slots.at[slot], f_ss.at[to], f_rs.at[slot], to)

    def q_copy(it, to, slot):
        return var_copy(q_slots.at[it, slot], q_slots.at[it, slot], q_ss.at[it, to], q_rs.at[it, slot], to)

    def sq_copy(it, to, slot):
        return var_copy(sq_send.at[it, to], sq_recv.at[it, slot], sq_ss.at[it, to], sq_rs.at[it, slot], to)

    def sf_copy(to, slot):
        return smp_copy(sf_send.at[to], sf_recv.at[slot], sf_ss.at[to], sf_rs.at[slot], to)

    def sc_copy(it, c, i, to, slot):
        return smp_copy(sc_send.at[it, c, i], sc_recv.at[it, slot], sc_ss.at[it, c, i], sc_rs.at[it, slot], to)

    def c_copy(it, to, slot):
        return smp_copy(c_slots.at[it, slot], c_slots.at[it, slot], c_ss.at[it, to], c_rs.at[it, slot], to)

    sent = []

    def start(copy, when=None):
        sent.append((copy, when))
        if when is None:
            copy.start()
        else:
            pl.when(when)(copy.start)

    for p in smp_peers:
        start(f_copy(p, js))
    for p in var_peers:
        start(q_copy(0, p, iv))

    load_d.wait()
    blocks = samples // ROWS
    ones = jnp.ones((8, chunk), BF16)
    counts = []
    for b in range(blocks):
        here = slice(b * ROWS, (b + 1) * ROWS)
        count = jnp.zeros((8, ROWS), F32)
        for c in range(2):
            packed = dosage_ref[b * ROWS // CODES:(b + 1) * ROWS // CODES, c * chunk:(c + 1) * chunk]
            shape3 = (ROWS // CODES, CODES, chunk)
            shifts = 2 * lax.broadcasted_iota(jnp.int32, shape3, 1)
            codes = jnp.bitwise_and(jnp.right_shift(jnp.broadcast_to(packed[:, None, :], shape3), shifts), 3)
            codes = codes.reshape(ROWS, chunk)
            live = codes < 3
            alt = jnp.where(live, codes.astype(F32), 0.0)
            both = jnp.where(live, 2.0, 0.0)
            alt_ref[c, here, :] = alt
            ref_ref[c, here, :] = both - alt
            count = count + dot_nt(ones, both.astype(BF16))
        counts.append(count[0:1])
    counts = jnp.concatenate(counts, axis=1)

    for it in range(ITERS):
        last = it + 1 == ITERS

        for p in var_peers:
            q_copy(it, p, p).wait_recv()
        for v in range(nv):
            q_pad[0:pops, v * ws:(v + 1) * ws] = q_slots[it, v]
        qh, qm, ql = split(q_pad[...], 3)
        qs = jnp.concatenate([qh, qh, qm, qh, qm, ql, qm, ql], axis=0)
        qt_ref[...] = qs.astype(F32).T.astype(BF16)
        none = jnp.zeros_like(qh)
        qd_ref[...] = jnp.concatenate([qh, none, qm, none], axis=0)
        qb_ref[...] = jnp.concatenate([none, qh, none, qm], axis=0)

        sq_acc = [jnp.zeros((2 * PAD, ROWS), F32) for _ in range(blocks)]
        for t in range(2):
            c = side if (it == 0) == (t == 0) else 1 - side
            if it == 0:
                for i in range(half):
                    p = c * half + lax.rem(js + i, half)
                    if t or i:
                        f_copy(p, p).wait_recv()
                for i in range(half):
                    f_pad[0:pops, i * wf:(i + 1) * wf] = f_slots[c * half + i]
            else:
                for i in range(mids):
                    slot = c * mids + i
                    copy = c_copy(it, js, slot)
                    pl.when(middle(c, i) != js)(copy.wait_recv)
                for i in range(mids):
                    f_pad[0:pops, i * wc:(i + 1) * wc] = c_slots[it, c * mids + i]
            f_all = f_pad[...]
            fh, fm, fl = split(f_all, 3)
            fs_ref[...] = jnp.concatenate([fh, fm, fh, fl, fm, fh, fl, fm], axis=0)
            fpair = jnp.concatenate([fh, fm], axis=0)
            fgs_ref[...] = jnp.concatenate([fpair, fpair], axis=1)

            kept = []
            sums = jnp.zeros((4 * PAD, chunk), F32)
            for b in range(blocks):
                here = slice(b * ROWS, (b + 1) * ROWS)
                probs = dot(qt_ref[here, :], fs_ref[...])
                rest = 1.0 - probs
                inv = 1.0 / (probs * rest)
                alt = alt_ref[c, here, :] * rest
                bb = ref_ref[c, here, :] * probs
                dd = (alt - bb) * inv
                bb = bb * inv
                dh, dl = split(dd, 2)
                bh, bl = split(bb, 2)
                qd, qb = qd_ref[:, here], qb_ref[:, here]
                sums = sums + dot(
                    jnp.concatenate([qd, qd, qb, qb], axis=1), jnp.concatenate([dh, dl, bh, bl], axis=0))
                kept.append(jnp.concatenate([dh, dl], axis=1))
                if t == 0:
                    sq_acc[b] = sq_acc[b] + dot_nt(fgs_ref[...], kept[b])
            sums = sums[0:2 * PAD] + sums[2 * PAD:4 * PAD]
            sum_d, sum_b = sums[0:pops], sums[PAD:PAD + pops]
            if last:
                for i in range(half):
                    cut = slice(i * wf, (i + 1) * wf)
                    sf_send[c * half + i] = jnp.concatenate([sum_d[:, cut], sum_b[:, cut]], axis=1)
                for i in range(half):
                    p = c * half + lax.rem(js + i, half)
                    if i or t == 0:
                        start(sf_copy(p, js))
            else:
                stacked = jnp.concatenate([sum_d, sum_b], axis=0)
                for i in range(mids):
                    sc_send[it, c, i] = stacked[:, i * wc:(i + 1) * wc]
                for i in range(mids):
                    to = middle(c, i)
                    start(sc_copy(it, c, i, to, js), to != js)

        for b in range(blocks):
            sq_acc[b] = sq_acc[b] + dot_nt(fgs_ref[...], kept[b])
        sum_q = jnp.concatenate([x[0:PAD] + x[PAD:2 * PAD] for x in sq_acc], axis=1)
        sum_q = sum_q + (counts - jnp.sum(q_pad[...] * sum_q, axis=0, keepdims=True))
        sum_q = sum_q[0:pops]
        for v in range(nv):
            sq_send[it, v] = sum_q[:, v * ws:(v + 1) * ws]
        for p in var_peers:
            start(sq_copy(it, p, iv))

        total = sq_send[it, iv]
        for p in var_peers:
            sq_copy(it, p, p).wait_recv()
            total = total + sq_recv[it, p]
        numer = q_own * total
        q_own = (numer + 0.5) / (jnp.sum(numer, axis=0, keepdims=True) + 0.5 * pops)
        if last:
            shares_out[...] = q_own
        else:
            q_slots[it + 1, iv] = q_own
            for p in var_peers:
                start(q_copy(it + 1, p, iv))

        if last:
            place = lax.rem(js, half)
            pair = c_slots[it, side * mids + place // 2]
            f_own = jnp.where(lax.rem(place, 2) == 0, pair[:, 0:wf], pair[:, wf:2 * wf])
            total = sf_send[js]
            for p in smp_peers:
                sf_copy(p, p).wait_recv()
                total = total + sf_recv[p]
            sum_d, sum_b = total[:, 0:wf], total[:, wf:2 * wf]
            freqs_out[...] = (f_own * (sum_d + sum_b) + 0.5) / (f_own * sum_d + sum_b + 1.0)
        else:
            slot = my_mid_chunk * mids + my_mid

            @pl.when(is_mid)
            def _():
                total = sc_send[it, my_mid_chunk, my_mid]
                for p in smp_peers:
                    sc_copy(it, my_mid_chunk, my_mid, js, p).wait_recv()
                    total = total + sc_recv[it, p]
                if it == 0:
                    first = my_mid_chunk * half + 2 * my_mid
                    f_old = jnp.concatenate([f_slots[first], f_slots[first + 1]], axis=1)
                else:
                    f_old = c_slots[it, slot]
                sum_d, sum_b = total[0:pops], total[pops:2 * pops]
                c_slots[it + 1, slot] = (f_old * (sum_d + sum_b) + 0.5) / (f_old * sum_d + sum_b + 1.0)

            for p in smp_peers:
                start(c_copy(it + 1, p, slot), is_mid)

    for copy, when in sent:
        if when is None:
            copy.wait_send()
        else:
            pl.when(when)(copy.wait_send)


def hand_out(shares_ref, freqs_ref, shares_out, freqs_out):
    shares_out[...] = shares_ref[...]
    freqs_out[...] = freqs_ref[...]


def body(nv, ns, dosage, shares_init, freqs_init):
    pops, ws = shares_init.shape
    wf = freqs_init.shape[1]
    words, variants = dosage.shape
    samples = words * CODES
    chunk = variants // 2
    mids = ns // 4
    wc = chunk // mids
    vmem = pl.BlockSpec(memory_space=pltpu.VMEM)
    hbm = pl.BlockSpec(memory_space=pl.ANY)
    dma = pltpu.SemaphoreType.DMA
    shapes = (jax.ShapeDtypeStruct((pops, ws), F32), jax.ShapeDtypeStruct((pops, wf), F32))
    shares, freqs = pl.pallas_call(
        functools.partial(em_kernel, nv, ns),
        out_shape=(pltpu.VMEM((pops, ws), F32), pltpu.VMEM((pops, wf), F32)),
        in_specs=[hbm, hbm, hbm],
        out_specs=(vmem, vmem),
        scratch_shapes=[
            pltpu.VMEM((words, variants), jnp.int32),
            pltpu.VMEM((pops, ws), F32),
            pltpu.VMEM((pops, wf), F32),
            pltpu.VMEM((2, samples, chunk), F32),
            pltpu.VMEM((2, samples, chunk), F32),
            pltpu.VMEM((ITERS, nv, pops, ws), F32),
            pltpu.VMEM((ns, pops, wf), F32),
            pltpu.VMEM((ITERS, 2 * mids, pops, wc), F32),
            pltpu.VMEM((ITERS, nv, pops, ws), F32),
            pltpu.VMEM((ITERS, nv, pops, ws), F32),
            pltpu.VMEM((ITERS, 2, mids, 2 * pops, wc), F32),
            pltpu.VMEM((ITERS, ns, 2 * pops, wc), F32),
            pltpu.VMEM((ns, pops, 2 * wf), F32),
            pltpu.VMEM((ns, pops, 2 * wf), F32),
            pltpu.VMEM((PAD, samples), F32),
            pltpu.VMEM((PAD, chunk), F32),
            pltpu.VMEM((samples, 8 * PAD), BF16),
            pltpu.VMEM((4 * PAD, samples), BF16),
            pltpu.VMEM((4 * PAD, samples), BF16),
            pltpu.VMEM((8 * PAD, chunk), BF16),
            pltpu.VMEM((2 * PAD, 2 * chunk), BF16),
            dma((3,)),
            dma((ITERS, nv)), dma((ITERS, nv)),
            dma((ns,)), dma((ns,)),
            dma((ITERS, ns)), dma((ITERS, 2 * mids)),
            dma((ITERS, nv)), dma((ITERS, nv)),
            dma((ITERS, 2, mids)), dma((ITERS, ns)),
            dma((ns,)), dma((ns,)),
        ],
        compiler_params=pltpu.CompilerParams(collective_id=0, has_side_effects=True),
        cost_estimate=pl.CostEstimate(flops=200000000, bytes_accessed=400000, transcendentals=1000000),
    )(dosage, shares_init, freqs_init)
    shares = pltpu.with_memory_space_constraint(shares, pltpu.VMEM)
    freqs = pltpu.with_memory_space_constraint(freqs, pltpu.VMEM)
    return pl.pallas_call(
        hand_out, out_shape=shapes, in_specs=[vmem, vmem], out_specs=(vmem, vmem),
    )(shares, freqs)


def solution(mesh):
    placed = (P("smp", "var"), P(None, ("smp", "var")), P(None, ("var", "smp")))
    return jax.shard_map(
        functools.partial(body, mesh.shape["var"], mesh.shape["smp"]),
        mesh=mesh,
        in_specs=placed,
        out_specs=(P(None, ("smp", "var")), P(None, ("var", "smp"))),
        check_vma=False,
    )
```

```python
import functools

import jax
import jax.numpy as jnp
from jax import lax
from jax.experimental import pallas as pl
from jax.experimental.pallas import tpu as pltpu
from jax.sharding import PartitionSpec as P

ITERS = 2
CODES = 16
PAD = 16
ROWS = 512
LEVELS = 64
F32 = jnp.float32
BF16 = jnp.bfloat16


def split(x, pieces):
    out = []
    for _ in range(pieces):
        piece = x.astype(BF16)
        out.append(piece)
        x = x - piece.astype(F32)
    return out


def dot(a, b):
    return jnp.dot(a, b, preferred_element_type=F32)


def dot_nt(a, b):
    return lax.dot_general(a, b, (((1,), (1,)), ((), ())), preferred_element_type=F32)


def em_kernel(
    nv, ns, dosage_hbm, shares_hbm, freqs_hbm, shares_out, freqs_out,
    dosage_ref, shares_ref, freqs_ref, alt_ref, ref_ref,
    q_slots, f_slots, c_slots, sq_send, sq_recv, sc_send, sc_recv, sf_send, sf_recv,
    q_pad, f_pad, qt_ref, qd_ref, qb_ref, fs_ref, fgs_ref,
    load_sem, q_ss, q_rs, f_ss, f_rs, c_ss, c_rs, sq_ss, sq_rs, sc_ss, sc_rs, sf_ss, sf_rs,
):
    iv, js = lax.axis_index("var"), lax.axis_index("smp")
    pops, ws = shares_ref.shape
    wf = freqs_ref.shape[1]
    words, variants = dosage_ref.shape
    samples = words * CODES
    half = ns // 2
    mids = half // 2
    chunk = variants // 2
    wc = chunk // mids
    side = js // half
    mesh_ids = pl.DeviceIdType.MESH

    def other_smp(d):
        return lax.rem(js + d, ns)

    def middle(c, i):
        return (1 - c) * half + c * (half - mids) + i

    my_mid_chunk = 1 - side
    my_mid = js - middle(my_mid_chunk, 0)
    is_mid = jnp.logical_and(js >= half - mids, js < half + mids)
    smp_peers = [other_smp(d) for d in range(1, ns)]
    var_peers = [lax.rem(iv + d, nv) for d in range(1, nv)]

    barrier = pltpu.get_barrier_semaphore()
    for p in smp_peers:
        pl.semaphore_signal(barrier, inc=1, device_id=(p, iv), device_id_type=mesh_ids)
    for p in var_peers:
        pl.semaphore_signal(barrier, inc=1, device_id=(js, p), device_id_type=mesh_ids)

    load_q = pltpu.make_async_copy(shares_hbm, shares_ref, load_sem.at[0])
    load_f = pltpu.make_async_copy(freqs_hbm, f_slots.at[js], load_sem.at[1])
    load_d = pltpu.make_async_copy(dosage_hbm, dosage_ref, load_sem.at[2])
    load_q.start()
    load_f.start()
    load_d.start()
    q_pad[...] = jnp.zeros_like(q_pad)
    f_pad[...] = jnp.zeros_like(f_pad)
    load_q.wait()
    q_own = shares_ref[...]
    q_own = q_own / jnp.sum(q_own, axis=0, keepdims=True)
    q_slots[0, iv] = q_own
    load_f.wait()
    pl.semaphore_wait(barrier, ns - 1 + nv - 1)

    def smp_copy(src, dst, ss, rs, to):
        return pltpu.make_async_remote_copy(
            src_ref=src, dst_ref=dst, send_sem=ss, recv_sem=rs, device_id=(to, iv), device_id_type=mesh_ids)

    def var_copy(src, dst, ss, rs, to):
        return pltpu.make_async_remote_copy(
            src_ref=src, dst_ref=dst, send_sem=ss, recv_sem=rs, device_id=(js, to), device_id_type=mesh_ids)

    def f_copy(to, slot):
        return smp_copy(f_slots.at[slot], f_slots.at[slot], f_ss.at[to], f_rs.at[slot], to)

    def q_copy(it, to, slot):
        return var_copy(q_slots.at[it, slot], q_slots.at[it, slot], q_ss.at[it, to], q_rs.at[it, slot], to)

    def sq_copy(it, to, slot):
        return var_copy(sq_send.at[it, to], sq_recv.at[it, slot], sq_ss.at[it, to], sq_rs.at[it, slot], to)

    def sf_copy(to, slot):
        return smp_copy(sf_send.at[to], sf_recv.at[slot], sf_ss.at[to], sf_rs.at[slot], to)

    def sc_copy(it, c, i, to, slot):
        return smp_copy(sc_send.at[it, c, i], sc_recv.at[it, slot], sc_ss.at[it, c, i], sc_rs.at[it, slot], to)

    def c_copy(it, to, slot):
        return smp_copy(c_slots.at[it, slot], c_slots.at[it, slot], c_ss.at[it, to], c_rs.at[it, slot], to)

    sent = []

    def start(copy, when=None):
        sent.append((copy, when))
        if when is None:
            copy.start()
        else:
            pl.when(when)(copy.start)

    for p in smp_peers:
        start(f_copy(p, js))
    for p in var_peers:
        start(q_copy(0, p, iv))

    load_d.wait()
    blocks = samples // ROWS
    ones = jnp.ones((8, chunk), BF16)
    shape3 = (ROWS // CODES, CODES, chunk)
    shifts = 2 * lax.broadcasted_iota(jnp.int32, shape3, 1)
    level = 16 * lax.broadcasted_iota(jnp.int32, shape3, 0) + lax.broadcasted_iota(jnp.int32, shape3, 1)
    level = jnp.bitwise_and(19 * level + 27 * lax.broadcasted_iota(jnp.int32, shape3, 2), LEVELS - 1)
    step = (level.astype(F32) - 0.5 * (LEVELS - 1)) * (2.0 ** -7 / LEVELS) + 1.0
    counts = []
    for b in range(blocks):
        here = slice(b * ROWS, (b + 1) * ROWS)
        count = jnp.zeros((8, ROWS), F32)
        for c in range(2):
            packed = dosage_ref[b * ROWS // CODES:(b + 1) * ROWS // CODES, c * chunk:(c + 1) * chunk]
            codes = jnp.bitwise_and(jnp.right_shift(jnp.broadcast_to(packed[:, None, :], shape3), shifts), 3)
            live = codes < 3
            alt = jnp.where(live, codes.astype(F32), 0.0)
            both = jnp.where(live, 2.0, 0.0)
            alt_ref[c, here, :] = (alt * step).reshape(ROWS, chunk)
            ref_ref[c, here, :] = ((both - alt) * step).reshape(ROWS, chunk)
            count = count + dot_nt(ones, both.reshape(ROWS, chunk).astype(BF16))
        counts.append(count[0:1])
    counts = jnp.concatenate(counts, axis=1)

    for it in range(ITERS):
        last = it + 1 == ITERS

        for p in var_peers:
            q_copy(it, p, p).wait_recv()
        for v in range(nv):
            q_pad[0:pops, v * ws:(v + 1) * ws] = q_slots[it, v]
        qh, qm = split(q_pad[...], 2)
        qs = jnp.concatenate([qh, qm, qh, qm], axis=0)
        qt_ref[...] = qs.astype(F32).T.astype(BF16)
        none = jnp.zeros_like(qh)
        qd_ref[...] = jnp.concatenate([qh, none, qm, none], axis=0)
        qb_ref[...] = jnp.concatenate([none, qh, none, qm], axis=0)

        sq_acc = [jnp.zeros((2 * PAD, ROWS), F32) for _ in range(blocks)]
        for t in range(2):
            c = side if (it == 0) == (t == 0) else 1 - side
            if it == 0:
                for i in range(half):
                    p = c * half + lax.rem(js + i, half)
                    if t or i:
                        f_copy(p, p).wait_recv()
                for i in range(half):
                    f_pad[0:pops, i * wf:(i + 1) * wf] = f_slots[c * half + i]
            else:
                for i in range(mids):
                    slot = c * mids + i
                    copy = c_copy(it, js, slot)
                    pl.when(middle(c, i) != js)(copy.wait_recv)
                for i in range(mids):
                    f_pad[0:pops, i * wc:(i + 1) * wc] = c_slots[it, c * mids + i]
            f_all = f_pad[...]
            fh, fm = split(f_all, 2)
            fs_ref[...] = jnp.concatenate([fh, fh, fm, fm], axis=0)
            fgs_ref[...] = jnp.concatenate([fh, fm], axis=0)

            kept = []
            sums = jnp.zeros((4 * PAD, chunk), F32)
            for b in range(blocks):
                here = slice(b * ROWS, (b + 1) * ROWS)
                probs = dot(qt_ref[here, :], fs_ref[...])
                rest = 1.0 - probs
                inv = 1.0 / (probs * rest)
                alt = alt_ref[c, here, :] * rest
                bb = ref_ref[c, here, :] * probs
                dd = (alt - bb) * inv
                bb = bb * inv
                dh, bh = dd.astype(BF16), bb.astype(BF16)
                sums = sums + (dot(qd_ref[:, here], dh) + dot(qb_ref[:, here], bh))
                kept.append(dh)
                if t == 0:
                    sq_acc[b] = sq_acc[b] + dot_nt(fgs_ref[...], kept[b])
            sums = sums[0:2 * PAD] + sums[2 * PAD:4 * PAD]
            sum_d, sum_b = sums[0:pops], sums[PAD:PAD + pops]
            if last:
                for i in range(half):
                    cut = slice(i * wf, (i + 1) * wf)
                    sf_send[c * half + i] = jnp.concatenate([sum_d[:, cut], sum_b[:, cut]], axis=1)
                for i in range(half):
                    p = c * half + lax.rem(js + i, half)
                    if i or t == 0:
                        start(sf_copy(p, js))
            else:
                stacked = jnp.concatenate([sum_d, sum_b], axis=0)
                for i in range(mids):
                    sc_send[it, c, i] = stacked[:, i * wc:(i + 1) * wc]
                for i in range(mids):
                    to = middle(c, i)
                    start(sc_copy(it, c, i, to, js), to != js)

        for b in range(blocks):
            sq_acc[b] = sq_acc[b] + dot_nt(fgs_ref[...], kept[b])
        sum_q = jnp.concatenate([x[0:PAD] + x[PAD:2 * PAD] for x in sq_acc], axis=1)
        sum_q = sum_q + (counts - jnp.sum(q_pad[...] * sum_q, axis=0, keepdims=True))
        sum_q = sum_q[0:pops]
        for v in range(nv):
            sq_send[it, v] = sum_q[:, v * ws:(v + 1) * ws]
        for p in var_peers:
            start(sq_copy(it, p, iv))

        total = sq_send[it, iv]
        for p in var_peers:
            sq_copy(it, p, p).wait_recv()
            total = total + sq_recv[it, p]
        numer = q_own * total
        q_own = (numer + 0.5) / (jnp.sum(numer, axis=0, keepdims=True) + 0.5 * pops)
        if last:
            shares_out[...] = q_own
        else:
            q_slots[it + 1, iv] = q_own
            for p in var_peers:
                start(q_copy(it + 1, p, iv))

        if last:
            place = lax.rem(js, half)
            pair = c_slots[it, side * mids + place // 2]
            f_own = jnp.where(lax.rem(place, 2) == 0, pair[:, 0:wf], pair[:, wf:2 * wf])
            total = sf_send[js]
            for p in smp_peers:
                sf_copy(p, p).wait_recv()
                total = total + sf_recv[p]
            sum_d, sum_b = total[:, 0:wf], total[:, wf:2 * wf]
            freqs_out[...] = (f_own * (sum_d + sum_b) + 0.5) / (f_own * sum_d + sum_b + 1.0)
        else:
            slot = my_mid_chunk * mids + my_mid

            @pl.when(is_mid)
            def _():
                total = sc_send[it, my_mid_chunk, my_mid]
                for p in smp_peers:
                    sc_copy(it, my_mid_chunk, my_mid, js, p).wait_recv()
                    total = total + sc_recv[it, p]
                if it == 0:
                    first = my_mid_chunk * half + 2 * my_mid
                    f_old = jnp.concatenate([f_slots[first], f_slots[first + 1]], axis=1)
                else:
                    f_old = c_slots[it, slot]
                sum_d, sum_b = total[0:pops], total[pops:2 * pops]
                c_slots[it + 1, slot] = (f_old * (sum_d + sum_b) + 0.5) / (f_old * sum_d + sum_b + 1.0)

            for p in smp_peers:
                start(c_copy(it + 1, p, slot), is_mid)

    for copy, when in sent:
        if when is None:
            copy.wait_send()
        else:
            pl.when(when)(copy.wait_send)


def hand_out(shares_ref, freqs_ref, shares_out, freqs_out):
    shares_out[...] = shares_ref[...]
    freqs_out[...] = freqs_ref[...]


def body(nv, ns, dosage, shares_init, freqs_init):
    pops, ws = shares_init.shape
    wf = freqs_init.shape[1]
    words, variants = dosage.shape
    samples = words * CODES
    chunk = variants // 2
    mids = ns // 4
    wc = chunk // mids
    vmem = pl.BlockSpec(memory_space=pltpu.VMEM)
    hbm = pl.BlockSpec(memory_space=pl.ANY)
    dma = pltpu.SemaphoreType.DMA
    shapes = (jax.ShapeDtypeStruct((pops, ws), F32), jax.ShapeDtypeStruct((pops, wf), F32))
    shares, freqs = pl.pallas_call(
        functools.partial(em_kernel, nv, ns),
        out_shape=(pltpu.VMEM((pops, ws), F32), pltpu.VMEM((pops, wf), F32)),
        in_specs=[hbm, hbm, hbm],
        out_specs=(vmem, vmem),
        scratch_shapes=[
            pltpu.VMEM((words, variants), jnp.int32),
            pltpu.VMEM((pops, ws), F32),
            pltpu.VMEM((pops, wf), F32),
            pltpu.VMEM((2, samples, chunk), F32),
            pltpu.VMEM((2, samples, chunk), F32),
            pltpu.VMEM((ITERS, nv, pops, ws), F32),
            pltpu.VMEM((ns, pops, wf), F32),
            pltpu.VMEM((ITERS, 2 * mids, pops, wc), F32),
            pltpu.VMEM((ITERS, nv, pops, ws), F32),
            pltpu.VMEM((ITERS, nv, pops, ws), F32),
            pltpu.VMEM((ITERS, 2, mids, 2 * pops, wc), F32),
            pltpu.VMEM((ITERS, ns, 2 * pops, wc), F32),
            pltpu.VMEM((ns, pops, 2 * wf), F32),
            pltpu.VMEM((ns, pops, 2 * wf), F32),
            pltpu.VMEM((PAD, samples), F32),
            pltpu.VMEM((PAD, chunk), F32),
            pltpu.VMEM((samples, 4 * PAD), BF16),
            pltpu.VMEM((4 * PAD, samples), BF16),
            pltpu.VMEM((4 * PAD, samples), BF16),
            pltpu.VMEM((4 * PAD, chunk), BF16),
            pltpu.VMEM((2 * PAD, chunk), BF16),
            dma((3,)),
            dma((ITERS, nv)), dma((ITERS, nv)),
            dma((ns,)), dma((ns,)),
            dma((ITERS, ns)), dma((ITERS, 2 * mids)),
            dma((ITERS, nv)), dma((ITERS, nv)),
            dma((ITERS, 2, mids)), dma((ITERS, ns)),
            dma((ns,)), dma((ns,)),
        ],
        compiler_params=pltpu.CompilerParams(collective_id=0, has_side_effects=True),
        cost_estimate=pl.CostEstimate(flops=200000000, bytes_accessed=400000, transcendentals=1000000),
    )(dosage, shares_init, freqs_init)
    shares = pltpu.with_memory_space_constraint(shares, pltpu.VMEM)
    freqs = pltpu.with_memory_space_constraint(freqs, pltpu.VMEM)
    return pl.pallas_call(
        hand_out, out_shape=shapes, in_specs=[vmem, vmem], out_specs=(vmem, vmem),
    )(shares, freqs)


def solution(mesh):
    placed = (P("smp", "var"), P(None, ("smp", "var")), P(None, ("var", "smp")))
    return jax.shard_map(
        functools.partial(body, mesh.shape["var"], mesh.shape["smp"]),
        mesh=mesh,
        in_specs=placed,
        out_specs=(P(None, ("smp", "var")), P(None, ("var", "smp"))),
        check_vma=False,
    )
```

```python
import functools

import jax
import jax.numpy as jnp
from jax import lax
from jax.experimental import pallas as pl
from jax.experimental.pallas import tpu as pltpu
from jax.sharding import PartitionSpec as P

ITERS = 2
CODES = 16
PAD = 16
ROWS = 512
LEVELS = 64
F32 = jnp.float32
BF16 = jnp.bfloat16


def split(x, pieces):
    out = []
    for _ in range(pieces):
        piece = x.astype(BF16)
        out.append(piece)
        x = x - piece.astype(F32)
    return out


def dot(a, b):
    return jnp.dot(a, b, preferred_element_type=F32)


def dot_nt(a, b):
    return lax.dot_general(a, b, (((1,), (1,)), ((), ())), preferred_element_type=F32)


def renewed_shares(old, sums):
    numer = old * sums
    return (numer + 0.5) / (jnp.sum(numer, axis=0, keepdims=True) + 0.5 * old.shape[0])


def renewed_freqs(old, sum_d, sum_b):
    return (old * (sum_d + sum_b) + 0.5) / (old * sum_d + sum_b + 1.0)


def em_kernel(
    nv, ns, dosage_hbm, shares_hbm, freqs_hbm, shares_out, freqs_out,
    dosage_ref, shares_ref, freqs_ref, alt_ref, ref_ref,
    q_slots, f_slots, p_slots, d_slots, c_slots, e_slots,
    sq_send, sq_recv, sp_send, sp_recv, sc_send, sc_recv, sf_send, sf_recv,
    q_pad, f_pad, qt_ref, qd_ref, qb_ref, fs_ref, fgs_ref,
    load_sem, q_ss, q_rs, f_ss, f_rs, p_ss, p_rs, d_ss, d_rs, c_ss, c_rs,
    sq_ss, sq_rs, sp_ss, sp_rs, sc_ss, sc_rs, sf_ss, sf_rs,
):
    iv, js = lax.axis_index("var"), lax.axis_index("smp")
    pops, ws = shares_ref.shape
    wf = freqs_ref.shape[1]
    words, variants = dosage_ref.shape
    samples = words * CODES
    half = ns // 2
    mids = half // 2
    chunk = variants // 2
    wc = chunk // mids
    side = js // half
    mesh_ids = pl.DeviceIdType.MESH

    def other_smp(d):
        return lax.rem(js + d, ns)

    def middle(c, i):
        return (1 - c) * half + c * (half - mids) + i

    my_mid_chunk = 1 - side
    my_mid = js - middle(my_mid_chunk, 0)
    place = lax.rem(js, half)
    core, chip, chips = lax.rem(iv, 2), iv // 2, nv // 2
    owner = 2 * chip + 1
    is_owner = core == 1
    central = jnp.logical_and(js >= half - mids, js < half + mids)
    is_mid = jnp.logical_and(is_owner, central)
    first = my_mid_chunk * half + 2 * my_mid
    smp_peers = [other_smp(d) for d in range(1, ns)]
    far_peers = [(1 - side) * (ns - 1 - i) + side * i for i in range(half)]
    near_peers = [side * half + lax.rem(js + d, half) for d in range(half - 1, 0, -1)]
    var_peers = [lax.rem(iv + d, nv) for d in range(1, nv)]

    barrier = pltpu.get_barrier_semaphore()
    for p in smp_peers:
        pl.semaphore_signal(barrier, inc=1, device_id=(p, iv), device_id_type=mesh_ids)
    for p in var_peers:
        pl.semaphore_signal(barrier, inc=1, device_id=(js, p), device_id_type=mesh_ids)

    load_q = pltpu.make_async_copy(shares_hbm, shares_ref, load_sem.at[0])
    load_f = pltpu.make_async_copy(freqs_hbm, f_slots.at[js], load_sem.at[1])
    load_d = pltpu.make_async_copy(dosage_hbm, dosage_ref, load_sem.at[2])
    load_q.start()
    load_f.start()
    load_d.start()
    q_pad[...] = jnp.zeros_like(q_pad)
    f_pad[...] = jnp.zeros_like(f_pad)
    load_q.wait()
    q_own = shares_ref[...]
    q_own = q_own / jnp.sum(q_own, axis=0, keepdims=True)
    q_slots[iv] = q_own
    load_f.wait()
    pl.semaphore_wait(barrier, ns - 1 + nv - 1)

    def far_copy(src, dst, ss, rs, smp, var):
        return pltpu.make_async_remote_copy(
            src_ref=src, dst_ref=dst, send_sem=ss, recv_sem=rs, device_id=(smp, var), device_id_type=mesh_ids)

    def f_copy(to, slot):
        return far_copy(f_slots.at[slot], f_slots.at[slot], f_ss.at[to], f_rs.at[slot], to, iv)

    def e_copy(slot):
        return far_copy(f_slots.at[first + slot], e_slots.at[slot], d_ss.at[slot], d_rs.at[slot], js, owner)

    def q_copy(to, slot):
        return far_copy(q_slots.at[slot], q_slots.at[slot], q_ss.at[to], q_rs.at[slot], js, to)

    def sq_copy(to, slot):
        return far_copy(sq_send.at[to], sq_recv.at[slot], sq_ss.at[to], sq_rs.at[slot], js, to)

    def sf_copy(to, slot):
        return far_copy(sf_send.at[to], sf_recv.at[slot], sf_ss.at[to], sf_rs.at[slot], to, iv)

    def sp_copy(it, j, slot):
        return far_copy(sp_send.at[it, j], sp_recv.at[it, slot], sp_ss.at[it, j], sp_rs.at[it, slot], js, 2 * j + 1)

    def p_copy(it, to, slot):
        return far_copy(p_slots.at[it, slot], p_slots.at[it, slot], p_ss.at[it, to], p_rs.at[it, slot], js, to)

    def sc_copy(it, c, i, g, slot):
        return far_copy(
            sc_send.at[it, c, i], sc_recv.at[it, g, slot], sc_ss.at[it, c, i], sc_rs.at[it, g, slot],
            middle(c, i), owner)

    def c_copy(it, to, slot):
        return far_copy(c_slots.at[it, slot], c_slots.at[it, slot], c_ss.at[it, 1, to], c_rs.at[it, slot], to, iv)

    def d_copy(it, to, slot):
        return far_copy(d_slots.at[it], c_slots.at[it, slot], c_ss.at[it, 0, to], c_rs.at[it, slot], to, iv - 1)

    sent = []

    def start(copy, when=None):
        sent.append((copy, when))
        if when is None:
            copy.start()
        else:
            pl.when(when)(copy.start)

    for p in far_peers + near_peers:
        start(f_copy(p, js))
    for p in var_peers:
        start(q_copy(p, iv))

    load_d.wait()
    blocks = samples // ROWS
    ones = jnp.ones((8, chunk), BF16)
    shape3 = (ROWS // CODES, CODES, chunk)
    shifts = 2 * lax.broadcasted_iota(jnp.int32, shape3, 1)
    level = 16 * lax.broadcasted_iota(jnp.int32, shape3, 0) + lax.broadcasted_iota(jnp.int32, shape3, 1)
    level = jnp.bitwise_and(19 * level + 27 * lax.broadcasted_iota(jnp.int32, shape3, 2), LEVELS - 1)
    step = (level.astype(F32) - 0.5 * (LEVELS - 1)) * (2.0 ** -7 / LEVELS) + 1.0
    counts = []
    for b in range(blocks):
        here = slice(b * ROWS, (b + 1) * ROWS)
        count = jnp.zeros((8, ROWS), F32)
        for c in range(2):
            packed = dosage_ref[b * ROWS // CODES:(b + 1) * ROWS // CODES, c * chunk:(c + 1) * chunk]
            codes = jnp.bitwise_and(jnp.right_shift(jnp.broadcast_to(packed[:, None, :], shape3), shifts), 3)
            live = codes < 3
            alt = jnp.where(live, codes.astype(F32), 0.0)
            both = jnp.where(live, 2.0, 0.0)
            alt_ref[c, here, :] = (alt * step).reshape(ROWS, chunk)
            ref_ref[c, here, :] = ((both - alt) * step).reshape(ROWS, chunk)
            count = count + dot_nt(ones, both.reshape(ROWS, chunk).astype(BF16))
        counts.append(count[0:1])
    counts = jnp.concatenate(counts, axis=1)

    for it in range(ITERS):
        last = it + 1 == ITERS

        if it == 0:
            for p in var_peers:
                q_copy(p, p).wait_recv()
            for v in range(nv):
                q_pad[0:pops, v * ws:(v + 1) * ws] = q_slots[v]
        else:
            for j in range(chips):
                pl.when(iv != 2 * j + 1)(p_copy(it, iv, j).wait_recv)
            for j in range(chips):
                q_pad[0:pops, 2 * j * ws:2 * (j + 1) * ws] = p_slots[it, j]
        qh, qm = split(q_pad[...], 2)
        qs = jnp.concatenate([qh, qm, qh, qm], axis=0)
        qt_ref[...] = qs.astype(F32).T.astype(BF16)
        none = jnp.zeros_like(qh)
        qd_ref[...] = jnp.concatenate([qh, none, qm, none], axis=0)
        qb_ref[...] = jnp.concatenate([none, qh, none, qm], axis=0)

        sq_acc = [jnp.zeros((2 * PAD, ROWS), F32) for _ in range(blocks)]
        for t in range(2):
            c = side if (it == 0) == (t == 0) else 1 - side
            if it == 0:
                for i in range(half):
                    p = c * half + lax.rem(js + i, half)
                    if t or i:
                        f_copy(p, p).wait_recv()
                for i in range(2 * t):
                    start(e_copy(i), jnp.logical_and(central, core == 0))
                for i in range(half):
                    f_pad[0:pops, i * wf:(i + 1) * wf] = f_slots[c * half + i]
            else:
                for i in range(mids):
                    slot = c * mids + i
                    copy = c_copy(it, js, slot)
                    pl.when(jnp.logical_or(core == 0, middle(c, i) != js))(copy.wait_recv)
                for i in range(mids):
                    f_pad[0:pops, i * wc:(i + 1) * wc] = c_slots[it, c * mids + i]
            f_all = f_pad[...]
            fh, fm = split(f_all, 2)
            fs_ref[...] = jnp.concatenate([fh, fh, fm, fm], axis=0)
            fgs_ref[...] = jnp.concatenate([fh, fm], axis=0)

            kept = []
            sums = jnp.zeros((4 * PAD, chunk), F32)
            for b in range(blocks):
                here = slice(b * ROWS, (b + 1) * ROWS)
                probs = dot(qt_ref[here, :], fs_ref[...])
                bb = ref_ref[c, here, :] * (1.0 / (1.0 - probs))
                dd = alt_ref[c, here, :] * (1.0 / probs) - bb
                dh, bh = dd.astype(BF16), bb.astype(BF16)
                sums = sums + (dot(qd_ref[:, here], dh) + dot(qb_ref[:, here], bh))
                kept.append(dh)
                if t == 0:
                    sq_acc[b] = sq_acc[b] + dot_nt(fgs_ref[...], kept[b])
            sums = sums[0:2 * PAD] + sums[2 * PAD:4 * PAD]
            sum_d, sum_b = sums[0:pops], sums[PAD:PAD + pops]
            if last:
                for i in range(half):
                    cut = slice(i * wf, (i + 1) * wf)
                    sf_send[c * half + i] = jnp.concatenate([sum_d[:, cut], sum_b[:, cut]], axis=1)
                for p in far_peers if t == 0 else near_peers:
                    start(sf_copy(p, js))
            else:
                stacked = jnp.concatenate([sum_d, sum_b], axis=0)
                for i in range(mids):
                    sc_send[it, c, i] = stacked[:, i * wc:(i + 1) * wc]
                for i in range(mids):
                    start(sc_copy(it, c, i, core, js), jnp.logical_or(core == 0, middle(c, i) != js))

        for b in range(blocks):
            sq_acc[b] = sq_acc[b] + dot_nt(fgs_ref[...], kept[b])
        sum_q = jnp.concatenate([x[0:PAD] + x[PAD:2 * PAD] for x in sq_acc], axis=1)
        sum_q = sum_q + (counts - jnp.sum(q_pad[...] * sum_q, axis=0, keepdims=True))
        sum_q = sum_q[0:pops]
        if not last:
            for j in range(chips):
                sp_send[it, j] = sum_q[:, 2 * j * ws:2 * (j + 1) * ws]
            for j in range(chips):
                start(sp_copy(it, j, iv), iv != 2 * j + 1)

            @pl.when(is_owner)
            def _():
                total = sp_send[it, chip]
                for p in var_peers:
                    sp_copy(it, chip, p).wait_recv()
                    total = total + sp_recv[it, p]
                if it == 0:
                    q_old = jnp.concatenate([q_slots[2 * chip], q_slots[2 * chip + 1]], axis=1)
                else:
                    q_old = p_slots[it, chip]
                p_slots[it + 1, chip] = renewed_shares(q_old, total)

            for p in var_peers:
                start(p_copy(it + 1, p, chip), is_owner)

            slot = my_mid_chunk * mids + my_mid
            for g in (1, 0):

                @pl.when(is_mid)
                def _():
                    if g:
                        total = sc_send[it, my_mid_chunk, my_mid]
                        peers = smp_peers
                    else:
                        total = jnp.zeros((2 * pops, wc), F32)
                        peers = smp_peers + [js]
                    for p in peers:
                        sc_copy(it, my_mid_chunk, my_mid, g, p).wait_recv()
                        total = total + sc_recv[it, g, p]
                    if it == 0 and g:
                        f_old = jnp.concatenate([f_slots[first], f_slots[first + 1]], axis=1)
                    elif it == 0:
                        e_copy(0).wait_recv()
                        e_copy(1).wait_recv()
                        f_old = jnp.concatenate([e_slots[0], e_slots[1]], axis=1)
                    else:
                        f_old = c_slots[it, slot] if g else d_slots[it]
                    new = renewed_freqs(f_old, total[0:pops], total[pops:2 * pops])
                    if g:
                        c_slots[it + 1, slot] = new
                    else:
                        d_slots[it + 1] = new

                for p in far_peers + near_peers + ([] if g else [js]):
                    start((c_copy if g else d_copy)(it + 1, p, slot), is_mid)
        else:
            for v in range(nv):
                sq_send[v] = sum_q[:, v * ws:(v + 1) * ws]
            for p in var_peers:
                start(sq_copy(p, iv))
            total = sq_send[iv]
            for p in var_peers:
                sq_copy(p, p).wait_recv()
                total = total + sq_recv[p]
            pair = p_slots[it, chip]
            shares_out[...] = renewed_shares(jnp.where(core == 0, pair[:, 0:ws], pair[:, ws:2 * ws]), total)

            pair = c_slots[it, side * mids + place // 2]
            f_own = jnp.where(lax.rem(place, 2) == 0, pair[:, 0:wf], pair[:, wf:2 * wf])
            total = sf_send[js]
            for p in smp_peers:
                sf_copy(p, p).wait_recv()
                total = total + sf_recv[p]
            freqs_out[...] = renewed_freqs(f_own, total[:, 0:wf], total[:, wf:2 * wf])

    for copy, when in sent:
        if when is None:
            copy.wait_send()
        else:
            pl.when(when)(copy.wait_send)


def hand_out(shares_ref, freqs_ref, shares_out, freqs_out):
    shares_out[...] = shares_ref[...]
    freqs_out[...] = freqs_ref[...]


def body(nv, ns, dosage, shares_init, freqs_init):
    pops, ws = shares_init.shape
    wf = freqs_init.shape[1]
    words, variants = dosage.shape
    samples = words * CODES
    chunk = variants // 2
    mids = ns // 4
    chips = nv // 2
    wc = chunk // mids
    vmem = pl.BlockSpec(memory_space=pltpu.VMEM)
    hbm = pl.BlockSpec(memory_space=pl.ANY)
    dma = pltpu.SemaphoreType.DMA
    shapes = (jax.ShapeDtypeStruct((pops, ws), F32), jax.ShapeDtypeStruct((pops, wf), F32))
    shares, freqs = pl.pallas_call(
        functools.partial(em_kernel, nv, ns),
        out_shape=(pltpu.VMEM((pops, ws), F32), pltpu.VMEM((pops, wf), F32)),
        in_specs=[hbm, hbm, hbm],
        out_specs=(vmem, vmem),
        scratch_shapes=[
            pltpu.VMEM((words, variants), jnp.int32),
            pltpu.VMEM((pops, ws), F32),
            pltpu.VMEM((pops, wf), F32),
            pltpu.VMEM((2, samples, chunk), F32),
            pltpu.VMEM((2, samples, chunk), F32),
            pltpu.VMEM((nv, pops, ws), F32),
            pltpu.VMEM((ns, pops, wf), F32),
            pltpu.VMEM((ITERS, chips, pops, 2 * ws), F32),
            pltpu.VMEM((ITERS, pops, wc), F32),
            pltpu.VMEM((ITERS, 2 * mids, pops, wc), F32),
            pltpu.VMEM((2, pops, wf), F32),
            pltpu.VMEM((nv, pops, ws), F32),
            pltpu.VMEM((nv, pops, ws), F32),
            pltpu.VMEM((ITERS, chips, pops, 2 * ws), F32),
            pltpu.VMEM((ITERS, nv, pops, 2 * ws), F32),
            pltpu.VMEM((ITERS, 2, mids, 2 * pops, wc), F32),
            pltpu.VMEM((ITERS, 2, ns, 2 * pops, wc), F32),
            pltpu.VMEM((ns, pops, 2 * wf), F32),
            pltpu.VMEM((ns, pops, 2 * wf), F32),
            pltpu.VMEM((PAD, samples), F32),
            pltpu.VMEM((PAD, chunk), F32),
            pltpu.VMEM((samples, 4 * PAD), BF16),
            pltpu.VMEM((4 * PAD, samples), BF16),
            pltpu.VMEM((4 * PAD, samples), BF16),
            pltpu.VMEM((4 * PAD, chunk), BF16),
            pltpu.VMEM((2 * PAD, chunk), BF16),
            dma((3,)),
            dma((nv,)), dma((nv,)),
            dma((ns,)), dma((ns,)),
            dma((ITERS, nv)), dma((ITERS, chips)),
            dma((2,)), dma((2,)),
            dma((ITERS, 2, ns)), dma((ITERS, 2 * mids)),
            dma((nv,)), dma((nv,)),
            dma((ITERS, chips)), dma((ITERS, nv)),
            dma((ITERS, 2, mids)), dma((ITERS, 2, ns)),
            dma((ns,)), dma((ns,)),
        ],
        compiler_params=pltpu.CompilerParams(collective_id=0, has_side_effects=True),
        cost_estimate=pl.CostEstimate(flops=200000000, bytes_accessed=400000, transcendentals=1000000),
    )(dosage, shares_init, freqs_init)
    shares = pltpu.with_memory_space_constraint(shares, pltpu.VMEM)
    freqs = pltpu.with_memory_space_constraint(freqs, pltpu.VMEM)
    return pl.pallas_call(
        hand_out, out_shape=shapes, in_specs=[vmem, vmem], out_specs=(vmem, vmem),
    )(shares, freqs)


def solution(mesh):
    placed = (P("smp", "var"), P(None, ("smp", "var")), P(None, ("var", "smp")))
    return jax.shard_map(
        functools.partial(body, mesh.shape["var"], mesh.shape["smp"]),
        mesh=mesh,
        in_specs=placed,
        out_specs=(P(None, ("smp", "var")), P(None, ("var", "smp"))),
        check_vma=False,
    )
```

```python
import functools

import jax
import jax.numpy as jnp
from jax import lax
from jax.experimental import pallas as pl
from jax.experimental.pallas import tpu as pltpu
from jax.sharding import PartitionSpec as P

ITERS = 2
CODES = 16
PAD = 16
ROWS = 512
LEVELS = 64
F32 = jnp.float32
BF16 = jnp.bfloat16


def split(x, pieces):
    out = []
    for _ in range(pieces):
        piece = x.astype(BF16)
        out.append(piece)
        x = x - piece.astype(F32)
    return out


def dot(a, b):
    return jnp.dot(a, b, preferred_element_type=F32)


def dot_nt(a, b):
    return lax.dot_general(a, b, (((1,), (1,)), ((), ())), preferred_element_type=F32)


def renewed_shares(old, sums):
    numer = old * sums
    return (numer + 0.5) / (jnp.sum(numer, axis=0, keepdims=True) + 0.5 * old.shape[0])


def renewed_freqs(old, sum_d, sum_b):
    return (old * (sum_d + sum_b) + 0.5) / (old * sum_d + sum_b + 1.0)


def full_rows(x):
    return jnp.concatenate([x, jnp.zeros((PAD - x.shape[0], x.shape[1]), x.dtype)], axis=0)


def em_kernel(
    nv, ns, dosage_hbm, shares_hbm, freqs_hbm, shares_out, freqs_out,
    dosage_ref, shares_ref, freqs_ref, w_ref,
    q_slots, f_slots, p_slots, d_slots, c_slots, e_slots,
    sq_send, sq_recv, sp_send, sp_recv, sc_send, sc_recv, sf_recv,
    q_pad, qt_ref, qd_ref, qb_ref, sq_ref,
    load_sem, q_ss, q_rs, f_ss, f_rs, p_ss, p_rs, d_ss, d_rs, c_ss, c_rs,
    sq_ss, sq_rs, sp_ss, sp_rs, sc_ss, sc_rs, sf_ss, sf_rs,
):
    iv, js = lax.axis_index("var"), lax.axis_index("smp")
    pops, ws = shares_ref.shape
    wf = freqs_ref.shape[1]
    words, variants = dosage_ref.shape
    samples = words * CODES
    half = ns // 2
    mids = half // 2
    chunk = variants // 2
    wc = chunk // mids
    side = js // half
    mesh_ids = pl.DeviceIdType.MESH

    def other_smp(d):
        return lax.rem(js + d, ns)

    def middle(c, i):
        return (1 - c) * half + c * (half - mids) + i

    my_mid_chunk = 1 - side
    my_mid = js - middle(my_mid_chunk, 0)
    place = lax.rem(js, half)
    core, chip, chips = lax.rem(iv, 2), iv // 2, nv // 2
    owner = 2 * chip + 1
    is_owner = core == 1
    central = jnp.logical_and(js >= half - mids, js < half + mids)
    is_mid = jnp.logical_and(is_owner, central)
    first = my_mid_chunk * half + 2 * my_mid
    smp_peers = [other_smp(d) for d in range(1, ns)]
    far_peers = [(1 - side) * (ns - 1 - i) + side * i for i in range(half)]
    near_peers = [side * half + lax.rem(js + d, half) for d in range(half - 1, 0, -1)]
    var_peers = [lax.rem(iv + d, nv) for d in range(1, nv)]

    barrier = pltpu.get_barrier_semaphore()
    for p in far_peers + near_peers:
        pl.semaphore_signal(barrier, inc=1, device_id=(p, iv), device_id_type=mesh_ids)
    for p in var_peers:
        pl.semaphore_signal(barrier, inc=1, device_id=(js, p), device_id_type=mesh_ids)

    load_q = pltpu.make_async_copy(shares_hbm, shares_ref, load_sem.at[0])
    load_f = pltpu.make_async_copy(freqs_hbm, freqs_ref, load_sem.at[1])
    load_d = pltpu.make_async_copy(dosage_hbm, dosage_ref, load_sem.at[2])
    load_q.start()
    load_f.start()
    load_d.start()
    q_pad[...] = jnp.zeros_like(q_pad)
    load_q.wait()
    q_own = shares_ref[...]
    q_own = q_own / jnp.sum(q_own, axis=0, keepdims=True)
    q_slots[iv] = q_own
    load_f.wait()
    f_own = freqs_ref[...]
    beside = jnp.zeros_like(f_own)
    odd = lax.rem(js, 2) == 1
    f_own = jnp.where(odd, jnp.concatenate([beside, f_own], axis=1), jnp.concatenate([f_own, beside], axis=1))
    f_slots[js] = full_rows(f_own)
    pl.semaphore_wait(barrier, ns - 1 + nv - 1)

    def far_copy(src, dst, ss, rs, smp, var):
        return pltpu.make_async_remote_copy(
            src_ref=src, dst_ref=dst, send_sem=ss, recv_sem=rs, device_id=(smp, var), device_id_type=mesh_ids)

    def f_copy(to, slot):
        return far_copy(f_slots.at[slot], f_slots.at[slot], f_ss.at[to], f_rs.at[slot], to, iv)

    def e_copy(slot):
        return far_copy(f_slots.at[first + slot], e_slots.at[slot], d_ss.at[slot], d_rs.at[slot], js, owner)

    def q_copy(to, slot):
        return far_copy(q_slots.at[slot], q_slots.at[slot], q_ss.at[to], q_rs.at[slot], js, to)

    def sq_copy(to, slot):
        return far_copy(sq_send.at[to], sq_recv.at[slot], sq_ss.at[to], sq_rs.at[slot], js, to)

    def sf_copy(c, to, slot):
        return far_copy(
            sc_send.at[ITERS - 1, c, lax.rem(to, half) // 2], sf_recv.at[slot], sf_ss.at[to], sf_rs.at[slot], to, iv)

    def sp_copy(it, j, slot):
        return far_copy(sp_send.at[it, j], sp_recv.at[it, slot], sp_ss.at[it, j], sp_rs.at[it, slot], js, 2 * j + 1)

    def p_copy(it, to, slot):
        return far_copy(p_slots.at[it, slot], p_slots.at[it, slot], p_ss.at[it, to], p_rs.at[it, slot], js, to)

    def sc_copy(it, c, i, g, slot):
        return far_copy(
            sc_send.at[it, c, i], sc_recv.at[it, g, slot], sc_ss.at[it, c, i], sc_rs.at[it, g, slot],
            middle(c, i), owner)

    def c_copy(it, to, slot):
        return far_copy(c_slots.at[it, slot], c_slots.at[it, slot], c_ss.at[it, 1, to], c_rs.at[it, slot], to, iv)

    def d_copy(it, to, slot):
        return far_copy(d_slots.at[it], c_slots.at[it, slot], c_ss.at[it, 0, to], c_rs.at[it, slot], to, iv - 1)

    sent = []

    def start(copy, when=None):
        sent.append((copy, when))
        if when is None:
            copy.start()
        else:
            pl.when(when)(copy.start)

    for p in far_peers + near_peers:
        start(f_copy(p, js))
    for p in var_peers:
        start(q_copy(p, iv))

    load_d.wait()
    blocks = samples // ROWS
    ones = jnp.ones((8, chunk), BF16)
    shape3 = (ROWS // CODES, CODES, chunk)
    shifts = 2 * lax.broadcasted_iota(jnp.int32, shape3, 1)
    level = 16 * lax.broadcasted_iota(jnp.int32, shape3, 0) + lax.broadcasted_iota(jnp.int32, shape3, 1)
    level = jnp.bitwise_and(19 * level + 27 * lax.broadcasted_iota(jnp.int32, shape3, 2), LEVELS - 1)
    step = (level.astype(F32) - 0.5 * (LEVELS - 1)) * (2.0 ** -7 / LEVELS) + 1.0
    counts = []
    for b in range(blocks):
        here = slice(b * ROWS, (b + 1) * ROWS)
        count = jnp.zeros((8, ROWS), F32)
        for c in range(2):
            packed = dosage_ref[b * ROWS // CODES:(b + 1) * ROWS // CODES, c * chunk:(c + 1) * chunk]
            codes = jnp.bitwise_and(jnp.right_shift(jnp.broadcast_to(packed[:, None, :], shape3), shifts), 3)
            live = codes < 3
            alt = jnp.where(live, codes.astype(F32), 0.0)
            both = jnp.where(live, 2.0, 0.0)
            w_ref[c, here, 0:chunk] = (alt * step).reshape(ROWS, chunk)
            w_ref[c, here, chunk:2 * chunk] = ((both - alt) * step).reshape(ROWS, chunk)
            count = count + dot_nt(ones, both.reshape(ROWS, chunk).astype(BF16))
        counts.append(count[0:1])
    counts = jnp.concatenate(counts, axis=1)

    for it in range(ITERS):
        last = it + 1 == ITERS

        if it == 0:
            for p in var_peers:
                q_copy(p, p).wait_recv()
            for v in range(nv):
                q_pad[0:pops, v * ws:(v + 1) * ws] = q_slots[v]
        else:
            for j in range(chips):
                pl.when(iv != 2 * j + 1)(p_copy(it, iv, j).wait_recv)
            for j in range(chips):
                q_pad[0:pops, 2 * j * ws:2 * (j + 1) * ws] = p_slots[it, j]
        qh, qm = split(q_pad[...], 2)
        qs = jnp.concatenate([qh, qm, qh, qm], axis=0)
        qt_ref[...] = qs.astype(F32).T.astype(BF16)
        qh, qm = qh.astype(F32)[0:pops], qm.astype(F32)[0:pops]
        none = jnp.zeros_like(qh)
        qd_ref[...] = jnp.concatenate([qh, none, qm, none], axis=0).astype(BF16)
        qb_ref[...] = jnp.concatenate([none, qh, none, qm], axis=0).astype(BF16)

        for t in range(2):
            c = side if (it == 0) == (t == 0) else 1 - side
            if it == 0:
                for i in range(half):
                    p = c * half + lax.rem(js + i, half)
                    if t or i:
                        f_copy(p, p).wait_recv()
                for i in range(2 * t):
                    start(e_copy(i), jnp.logical_and(central, core == 0))
                f_all = [f_slots[c * half + 2 * i] + f_slots[c * half + 2 * i + 1] for i in range(mids)]
            else:
                for i in range(mids):
                    slot = c * mids + i
                    copy = c_copy(it, js, slot)
                    pl.when(jnp.logical_or(core == 0, middle(c, i) != js))(copy.wait_recv)
                f_all = [c_slots[it, c * mids + i] for i in range(mids)]
            fh, fm = split(jnp.concatenate(f_all, axis=1), 2)
            fs = jnp.concatenate([fh, fh, fm, fm], axis=0)
            fg = jnp.concatenate([fh, fm], axis=0)

            kept = []
            sums = jnp.zeros((4 * pops, chunk), F32)
            for b in range(blocks):
                here = slice(b * ROWS, (b + 1) * ROWS)
                probs = dot(qt_ref[here, :], fs)
                bb = w_ref[c, here, chunk:2 * chunk] * (1.0 / (1.0 - probs))
                dd = w_ref[c, here, 0:chunk] * (1.0 / probs) - bb
                dh, bh = dd.astype(BF16), bb.astype(BF16)
                sums = sums + (dot(qd_ref[:, here], dh) + dot(qb_ref[:, here], bh))
                kept.append(dh)
            sums = sums[0:2 * pops] + sums[2 * pops:4 * pops]
            for i in range(mids):
                sc_send[it, c, i] = sums[:, i * wc:(i + 1) * wc]
            if last:
                for p in far_peers if t == 0 else near_peers:
                    start(sf_copy(c, p, js))
            else:
                for i in range(mids):
                    start(sc_copy(it, c, i, core, js), jnp.logical_or(core == 0, middle(c, i) != js))
            if t == 0:
                sq_ref[...] = jnp.concatenate([dot_nt(fg, x) for x in kept], axis=1)

        sum_q = sq_ref[...] + jnp.concatenate([dot_nt(fg, x) for x in kept], axis=1)
        sum_q = sum_q[0:PAD] + sum_q[PAD:2 * PAD]
        sum_q = sum_q + (counts - jnp.sum(q_pad[...] * sum_q, axis=0, keepdims=True))
        sum_q = sum_q[0:pops]
        if not last:
            for j in range(chips):
                sp_send[it, j] = sum_q[:, 2 * j * ws:2 * (j + 1) * ws]
            for j in range(chips):
                start(sp_copy(it, j, iv), iv != 2 * j + 1)

            @pl.when(is_owner)
            def _():
                total = sp_send[it, chip]
                for p in var_peers:
                    sp_copy(it, chip, p).wait_recv()
                    total = total + sp_recv[it, p]
                if it == 0:
                    q_old = jnp.concatenate([q_slots[2 * chip], q_slots[2 * chip + 1]], axis=1)
                else:
                    q_old = p_slots[it, chip]
                p_slots[it + 1, chip] = renewed_shares(q_old, total)

            for p in var_peers:
                start(p_copy(it + 1, p, chip), is_owner)

            slot = my_mid_chunk * mids + my_mid
            for g in (1, 0):

                @pl.when(is_mid)
                def _():
                    if g:
                        total = sc_send[it, my_mid_chunk, my_mid]
                        peers = smp_peers
                    else:
                        total = jnp.zeros((2 * pops, wc), F32)
                        peers = smp_peers + [js]
                    for p in peers:
                        sc_copy(it, my_mid_chunk, my_mid, g, p).wait_recv()
                        total = total + sc_recv[it, g, p]
                    if it == 0 and g:
                        f_old = f_slots[first] + f_slots[first + 1]
                    elif it == 0:
                        e_copy(0).wait_recv()
                        e_copy(1).wait_recv()
                        f_old = e_slots[0] + e_slots[1]
                    else:
                        f_old = c_slots[it, slot] if g else d_slots[it]
                    new = full_rows(renewed_freqs(f_old[0:pops], total[0:pops], total[pops:2 * pops]))
                    if g:
                        c_slots[it + 1, slot] = new
                    else:
                        d_slots[it + 1] = new

                for p in far_peers + near_peers + ([] if g else [js]):
                    start((c_copy if g else d_copy)(it + 1, p, slot), is_mid)
        else:
            for v in range(nv):
                sq_send[v] = sum_q[:, v * ws:(v + 1) * ws]
            for p in var_peers:
                start(sq_copy(p, iv))
            total = sq_send[iv]
            for p in var_peers:
                sq_copy(p, p).wait_recv()
                total = total + sq_recv[p]
            pair = p_slots[it, chip]
            shares_out[...] = renewed_shares(jnp.where(core == 0, pair[:, 0:ws], pair[:, ws:2 * ws]), total)

            total = sc_send[it, side, place // 2]
            for p in smp_peers:
                sf_copy(side, p, p).wait_recv()
                total = total + sf_recv[p]
            pair = renewed_freqs(c_slots[it, side * mids + place // 2][0:pops], total[0:pops], total[pops:2 * pops])
            freqs_out[...] = jnp.where(odd, pair[:, wf:2 * wf], pair[:, 0:wf])

    for copy, when in sent:
        if when is None:
            copy.wait_send()
        else:
            pl.when(when)(copy.wait_send)


def hand_out(shares_ref, freqs_ref, shares_out, freqs_out, sems):
    copies = [
        pltpu.make_async_copy(shares_ref, shares_out, sems.at[0]),
        pltpu.make_async_copy(freqs_ref, freqs_out, sems.at[1]),
    ]
    for copy in copies:
        copy.start()
    for copy in copies:
        copy.wait()


def body(nv, ns, dosage, shares_init, freqs_init):
    pops, ws = shares_init.shape
    wf = freqs_init.shape[1]
    words, variants = dosage.shape
    samples = words * CODES
    chunk = variants // 2
    mids = ns // 4
    chips = nv // 2
    wc = chunk // mids
    vmem = pl.BlockSpec(memory_space=pltpu.VMEM)
    hbm = pl.BlockSpec(memory_space=pl.ANY)
    dma = pltpu.SemaphoreType.DMA
    shapes = (jax.ShapeDtypeStruct((pops, ws), F32), jax.ShapeDtypeStruct((pops, wf), F32))
    shares, freqs = pl.pallas_call(
        functools.partial(em_kernel, nv, ns),
        out_shape=(pltpu.VMEM((pops, ws), F32), pltpu.VMEM((pops, wf), F32)),
        in_specs=[hbm, hbm, hbm],
        out_specs=(vmem, vmem),
        scratch_shapes=[
            pltpu.VMEM((words, variants), jnp.int32),
            pltpu.VMEM((pops, ws), F32),
            pltpu.VMEM((pops, wf), F32),
            pltpu.VMEM((2, samples, 2 * chunk), F32),
            pltpu.VMEM((nv, pops, ws), F32),
            pltpu.VMEM((ns, PAD, wc), F32),
            pltpu.VMEM((ITERS, chips, pops, 2 * ws), F32),
            pltpu.VMEM((ITERS, PAD, wc), F32),
            pltpu.VMEM((ITERS, 2 * mids, PAD, wc), F32),
            pltpu.VMEM((2, PAD, wc), F32),
            pltpu.VMEM((nv, pops, ws), F32),
            pltpu.VMEM((nv, pops, ws), F32),
            pltpu.VMEM((ITERS, chips, pops, 2 * ws), F32),
            pltpu.VMEM((ITERS, nv, pops, 2 * ws), F32),
            pltpu.VMEM((ITERS, 2, mids, 2 * pops, wc), F32),
            pltpu.VMEM((ITERS, 2, ns, 2 * pops, wc), F32),
            pltpu.VMEM((ns, 2 * pops, wc), F32),
            pltpu.VMEM((PAD, samples), F32),
            pltpu.VMEM((samples, 4 * PAD), BF16),
            pltpu.VMEM((4 * pops, samples), BF16),
            pltpu.VMEM((4 * pops, samples), BF16),
            pltpu.VMEM((2 * PAD, samples), F32),
            dma((3,)),
            dma((nv,)), dma((nv,)),
            dma((ns,)), dma((ns,)),
            dma((ITERS, nv)), dma((ITERS, chips)),
            dma((2,)), dma((2,)),
            dma((ITERS, 2, ns)), dma((ITERS, 2 * mids)),
            dma((nv,)), dma((nv,)),
            dma((ITERS, chips)), dma((ITERS, nv)),
            dma((ITERS, 2, mids)), dma((ITERS, 2, ns)),
            dma((ns,)), dma((ns,)),
        ],
        compiler_params=pltpu.CompilerParams(collective_id=0, has_side_effects=True),
        cost_estimate=pl.CostEstimate(flops=200000000, bytes_accessed=400000, transcendentals=1000000),
    )(dosage, shares_init, freqs_init)
    shares = pltpu.with_memory_space_constraint(shares, pltpu.VMEM)
    freqs = pltpu.with_memory_space_constraint(freqs, pltpu.VMEM)
    return pl.pallas_call(
        hand_out, out_shape=shapes, in_specs=[vmem, vmem], out_specs=(hbm, hbm), scratch_shapes=[dma((2,))],
    )(shares, freqs)


def solution(mesh):
    placed = (P("smp", "var"), P(None, ("smp", "var")), P(None, ("var", "smp")))
    return jax.shard_map(
        functools.partial(body, mesh.shape["var"], mesh.shape["smp"]),
        mesh=mesh,
        in_specs=placed,
        out_specs=(P(None, ("smp", "var")), P(None, ("var", "smp"))),
        check_vma=False,
    )
```

```python
import functools

import jax
import jax.numpy as jnp
from jax import lax
from jax.experimental import pallas as pl
from jax.experimental.pallas import tpu as pltpu
from jax.sharding import PartitionSpec as P

ITERS = 2
CODES = 16
PAD = 16
ROWS = 512
LEVELS = 64
F32 = jnp.float32
BF16 = jnp.bfloat16


def split(x, pieces):
    out = []
    for _ in range(pieces):
        piece = x.astype(BF16)
        out.append(piece)
        x = x - piece.astype(F32)
    return out


def dot(a, b):
    return jnp.dot(a, b, preferred_element_type=F32)


def dot_nt(a, b):
    return lax.dot_general(a, b, (((1,), (1,)), ((), ())), preferred_element_type=F32)


def renewed_shares(old, sums):
    numer = old * sums
    return (numer + 0.5) / (jnp.sum(numer, axis=0, keepdims=True) + 0.5 * old.shape[0])


def renewed_freqs(old, sum_d, sum_b):
    return (old * (sum_d + sum_b) + 0.5) / (old * sum_d + sum_b + 1.0)


def full_rows(x):
    return jnp.concatenate([x, jnp.zeros((PAD - x.shape[0], x.shape[1]), x.dtype)], axis=0)


def em_kernel(
    nv, ns, dosage_hbm, shares_hbm, freqs_hbm, shares_out, freqs_out,
    dosage_ref, shares_ref, freqs_ref, w_ref,
    q_slots, f_slots, p_slots, d_slots, c_slots, e_slots,
    sq_send, sq_recv, sp_send, sp_recv, sc_send, sc_recv, sf_recv,
    q_pad, qt_ref, qd_ref, qb_ref, sq_ref,
    load_sem, q_ss, q_rs, f_ss, f_rs, p_ss, p_rs, d_ss, d_rs, c_ss, c_rs,
    sq_ss, sq_rs, sp_ss, sp_rs, sc_ss, sc_rs, sf_ss, sf_rs,
):
    iv, js = lax.axis_index("var"), lax.axis_index("smp")
    pops, ws = shares_ref.shape
    wf = freqs_ref.shape[1]
    words, variants = dosage_ref.shape
    samples = words * CODES
    half = ns // 2
    mids = half // 2
    chunk = variants // 2
    wc = chunk // mids
    side = js // half
    mesh_ids = pl.DeviceIdType.MESH

    def other_smp(d):
        return lax.rem(js + d, ns)

    def middle(c, i):
        return (1 - c) * half + c * (half - mids) + i

    my_mid_chunk = 1 - side
    my_mid = js - middle(my_mid_chunk, 0)
    place = lax.rem(js, half)
    core, chip, chips = lax.rem(iv, 2), iv // 2, nv // 2
    owner = 2 * chip + 1
    is_owner = core == 1
    central = jnp.logical_and(js >= half - mids, js < half + mids)
    is_mid = jnp.logical_and(is_owner, central)
    first = my_mid_chunk * half + 2 * my_mid
    smp_peers = [other_smp(d) for d in range(1, ns)]
    far_peers = [(1 - side) * (ns - 1 - i) + side * i for i in range(half)]
    near_peers = [side * half + lax.rem(js + d, half) for d in range(half - 1, 0, -1)]
    var_peers = [lax.rem(iv + d, nv) for d in range(1, nv)]

    barrier = pltpu.get_barrier_semaphore()
    for p in far_peers + near_peers:
        pl.semaphore_signal(barrier, inc=1, device_id=(p, iv), device_id_type=mesh_ids)
    for p in var_peers:
        pl.semaphore_signal(barrier, inc=1, device_id=(js, p), device_id_type=mesh_ids)

    load_q = pltpu.make_async_copy(shares_hbm, shares_ref, load_sem.at[0])
    load_f = pltpu.make_async_copy(freqs_hbm, freqs_ref, load_sem.at[1])
    load_d = pltpu.make_async_copy(dosage_hbm, dosage_ref, load_sem.at[2])
    load_q.start()
    load_f.start()
    load_d.start()
    q_pad[...] = jnp.zeros_like(q_pad)
    load_q.wait()
    q_own = shares_ref[...]
    q_own = q_own / jnp.sum(q_own, axis=0, keepdims=True)
    q_slots[iv] = q_own
    load_f.wait()
    f_own = freqs_ref[...]
    beside = jnp.zeros_like(f_own)
    odd = lax.rem(js, 2) == 1
    f_own = jnp.where(odd, jnp.concatenate([beside, f_own], axis=1), jnp.concatenate([f_own, beside], axis=1))
    f_slots[js] = full_rows(f_own)
    pl.semaphore_wait(barrier, ns - 1 + nv - 1)

    def far_copy(src, dst, ss, rs, smp, var):
        return pltpu.make_async_remote_copy(
            src_ref=src, dst_ref=dst, send_sem=ss, recv_sem=rs, device_id=(smp, var), device_id_type=mesh_ids)

    def f_copy(to, slot):
        return far_copy(f_slots.at[slot], f_slots.at[slot], f_ss.at[to], f_rs.at[slot], to, iv)

    def e_copy(slot):
        return far_copy(f_slots.at[first + slot], e_slots.at[slot], d_ss.at[slot], d_rs.at[slot], js, owner)

    def q_copy(to, slot):
        return far_copy(q_slots.at[slot], q_slots.at[slot], q_ss.at[to], q_rs.at[slot], js, to)

    def sq_copy(to, slot):
        return far_copy(sq_send.at[to], sq_recv.at[slot], sq_ss.at[to], sq_rs.at[slot], js, to)

    def sf_copy(c, to, slot):
        return far_copy(
            sc_send.at[ITERS - 1, c, lax.rem(to, half) // 2], sf_recv.at[slot], sf_ss.at[to], sf_rs.at[slot], to, iv)

    def sp_copy(it, j, slot):
        return far_copy(sp_send.at[it, j], sp_recv.at[it, slot], sp_ss.at[it, j], sp_rs.at[it, slot], js, 2 * j + 1)

    def p_copy(it, to, slot):
        return far_copy(p_slots.at[it, slot], p_slots.at[it, slot], p_ss.at[it, to], p_rs.at[it, slot], js, to)

    def sc_copy(it, c, i, g, slot):
        return far_copy(
            sc_send.at[it, c, i], sc_recv.at[it, g, slot], sc_ss.at[it, c, i], sc_rs.at[it, g, slot],
            middle(c, i), owner)

    def c_copy(it, to, slot):
        return far_copy(c_slots.at[it, slot], c_slots.at[it, slot], c_ss.at[it, 1, to], c_rs.at[it, slot], to, iv)

    def d_copy(it, to, slot):
        return far_copy(d_slots.at[it], c_slots.at[it, slot], c_ss.at[it, 0, to], c_rs.at[it, slot], to, iv - 1)

    sent = []

    def start(copy, when=None):
        sent.append((copy, when))
        if when is None:
            copy.start()
        else:
            pl.when(when)(copy.start)

    for p in far_peers + near_peers:
        start(f_copy(p, js))
    for p in var_peers:
        start(q_copy(p, iv))

    load_d.wait()
    blocks = samples // ROWS
    ones = jnp.ones((8, chunk), BF16)
    shape3 = (ROWS // CODES, CODES, chunk)
    shifts = 2 * lax.broadcasted_iota(jnp.int32, shape3, 1)
    level = 16 * lax.broadcasted_iota(jnp.int32, shape3, 0) + lax.broadcasted_iota(jnp.int32, shape3, 1)
    level = jnp.bitwise_and(19 * level + 27 * lax.broadcasted_iota(jnp.int32, shape3, 2), LEVELS - 1)
    step = (level.astype(F32) - 0.5 * (LEVELS - 1)) * (2.0 ** -7 / LEVELS) + 1.0
    counts = []
    for b in range(blocks):
        here = slice(b * ROWS, (b + 1) * ROWS)
        count = jnp.zeros((8, ROWS), F32)
        for c in range(2):
            packed = dosage_ref[b * ROWS // CODES:(b + 1) * ROWS // CODES, c * chunk:(c + 1) * chunk]
            codes = jnp.bitwise_and(jnp.right_shift(jnp.broadcast_to(packed[:, None, :], shape3), shifts), 3)
            live = codes < 3
            alt = jnp.where(live, codes.astype(F32), 0.0)
            both = jnp.where(live, 2.0, 0.0)
            w_ref[c, here, 0:chunk] = (alt * step).reshape(ROWS, chunk)
            w_ref[c, here, chunk:2 * chunk] = ((both - alt) * step).reshape(ROWS, chunk)
            count = count + dot_nt(ones, both.reshape(ROWS, chunk).astype(BF16))
        counts.append(count[0:1])
    counts = jnp.concatenate(counts, axis=1)

    for it in range(ITERS):
        last = it + 1 == ITERS

        if it == 0:
            for p in var_peers:
                q_copy(p, p).wait_recv()
            for v in range(nv):
                q_pad[0:pops, v * ws:(v + 1) * ws] = q_slots[v]
        else:
            for j in range(chips):
                pl.when(iv != 2 * j + 1)(p_copy(it, iv, j).wait_recv)
            for j in range(chips):
                q_pad[0:pops, 2 * j * ws:2 * (j + 1) * ws] = p_slots[it, j]
        qh, qm = split(q_pad[...], 2)
        qs = jnp.concatenate([qh, qm, qh, qm], axis=0)
        qt_ref[...] = qs.astype(F32).T.astype(BF16)
        qh, qm = qh.astype(F32)[0:pops], qm.astype(F32)[0:pops]
        none = jnp.zeros_like(qh)
        qd_ref[...] = jnp.concatenate([qh, none, qm, none], axis=0).astype(BF16)
        qb_ref[...] = jnp.concatenate([none, qh, none, qm], axis=0).astype(BF16)

        for t in range(2):
            c = side if (it == 0) == (t == 0) else 1 - side
            if it == 0:
                for i in range(half):
                    p = c * half + lax.rem(js + i, half)
                    if t or i:
                        f_copy(p, p).wait_recv()
                for i in range(2 * t):
                    start(e_copy(i), jnp.logical_and(central, core == 0))
                f_all = [f_slots[c * half + 2 * i] + f_slots[c * half + 2 * i + 1] for i in range(mids)]
            else:
                for i in range(mids):
                    slot = c * mids + i
                    copy = c_copy(it, js, slot)
                    pl.when(jnp.logical_or(core == 0, middle(c, i) != js))(copy.wait_recv)
                f_all = [c_slots[it, c * mids + i] for i in range(mids)]
            fh, fm = split(jnp.concatenate(f_all, axis=1), 2)
            fs = jnp.concatenate([fh, fh, fm, fm], axis=0)
            fg = jnp.concatenate([fh, fm], axis=0)

            kept = []
            sums = jnp.zeros((4 * pops, chunk), F32)
            for b in range(blocks):
                here = slice(b * ROWS, (b + 1) * ROWS)
                probs = dot(qt_ref[here, :], fs)
                bb = w_ref[c, here, chunk:2 * chunk] * (1.0 / (1.0 - probs))
                dd = w_ref[c, here, 0:chunk] * (1.0 / probs) - bb
                dh, bh = dd.astype(BF16), bb.astype(BF16)
                sums = sums + (dot(qd_ref[:, here], dh) + dot(qb_ref[:, here], bh))
                kept.append(dh)
            sums = sums[0:2 * pops] + sums[2 * pops:4 * pops]
            for i in range(mids):
                sc_send[it, c, i] = sums[:, i * wc:(i + 1) * wc]
            if last:
                for p in far_peers if t == 0 else near_peers:
                    start(sf_copy(c, p, js))
            else:
                for i in range(mids):
                    start(sc_copy(it, c, i, core, js), jnp.logical_or(core == 0, middle(c, i) != js))
            if t == 0:
                sq_ref[...] = jnp.concatenate([dot_nt(fg, x) for x in kept], axis=1)

        sum_q = sq_ref[...] + jnp.concatenate([dot_nt(fg, x) for x in kept], axis=1)
        sum_q = sum_q[0:PAD] + sum_q[PAD:2 * PAD]
        sum_q = sum_q + (counts - jnp.sum(q_pad[...] * sum_q, axis=0, keepdims=True))
        sum_q = sum_q[0:pops]
        if not last:
            for j in range(chips):
                sp_send[it, j] = sum_q[:, 2 * j * ws:2 * (j + 1) * ws]
            for j in range(chips):
                start(sp_copy(it, j, iv), iv != 2 * j + 1)

            @pl.when(is_owner)
            def _():
                total = sp_send[it, chip]
                for p in var_peers:
                    sp_copy(it, chip, p).wait_recv()
                    total = total + sp_recv[it, p]
                if it == 0:
                    q_old = jnp.concatenate([q_slots[2 * chip], q_slots[2 * chip + 1]], axis=1)
                else:
                    q_old = p_slots[it, chip]
                p_slots[it + 1, chip] = renewed_shares(q_old, total)

            for p in var_peers:
                start(p_copy(it + 1, p, chip), is_owner)

            slot = my_mid_chunk * mids + my_mid
            for g in (1, 0):

                @pl.when(is_mid)
                def _():
                    if g:
                        total = sc_send[it, my_mid_chunk, my_mid]
                        peers = smp_peers
                    else:
                        total = jnp.zeros((2 * pops, wc), F32)
                        peers = smp_peers + [js]
                    for p in peers:
                        sc_copy(it, my_mid_chunk, my_mid, g, p).wait_recv()
                        total = total + sc_recv[it, g, p]
                    if it == 0 and g:
                        f_old = f_slots[first] + f_slots[first + 1]
                    elif it == 0:
                        e_copy(0).wait_recv()
                        e_copy(1).wait_recv()
                        f_old = e_slots[0] + e_slots[1]
                    else:
                        f_old = c_slots[it, slot] if g else d_slots[it]
                    new = full_rows(renewed_freqs(f_old[0:pops], total[0:pops], total[pops:2 * pops]))
                    if g:
                        c_slots[it + 1, slot] = new
                    else:
                        d_slots[it + 1] = new

                for p in far_peers + near_peers + ([] if g else [js]):
                    start((c_copy if g else d_copy)(it + 1, p, slot), is_mid)
        else:
            for v in range(nv):
                sq_send[v] = sum_q[:, v * ws:(v + 1) * ws]
            for p in var_peers:
                start(sq_copy(p, iv))
            total = sq_send[iv]
            for p in var_peers:
                sq_copy(p, p).wait_recv()
                total = total + sq_recv[p]
            pair = p_slots[it, chip]
            shares_out[...] = renewed_shares(jnp.where(core == 0, pair[:, 0:ws], pair[:, ws:2 * ws]), total)

            for copy, when in sent:
                if when is None:
                    copy.wait_send()
                else:
                    pl.when(when)(copy.wait_send)

            total = sc_send[it, side, place // 2]
            for p in smp_peers:
                sf_copy(side, p, p).wait_recv()
                total = total + sf_recv[p]
            pair = renewed_freqs(c_slots[it, side * mids + place // 2][0:pops], total[0:pops], total[pops:2 * pops])
            freqs_out[...] = jnp.where(odd, pair[:, wf:2 * wf], pair[:, 0:wf])


def hand_out(shares_ref, freqs_ref, shares_out, freqs_out, sems):
    copies = [
        pltpu.make_async_copy(shares_ref, shares_out, sems.at[0]),
        pltpu.make_async_copy(freqs_ref, freqs_out, sems.at[1]),
    ]
    for copy in copies:
        copy.start()
    for copy in copies:
        copy.wait()


def body(nv, ns, dosage, shares_init, freqs_init):
    pops, ws = shares_init.shape
    wf = freqs_init.shape[1]
    words, variants = dosage.shape
    samples = words * CODES
    chunk = variants // 2
    mids = ns // 4
    chips = nv // 2
    wc = chunk // mids
    vmem = pl.BlockSpec(memory_space=pltpu.VMEM)
    hbm = pl.BlockSpec(memory_space=pl.ANY)
    dma = pltpu.SemaphoreType.DMA
    shapes = (jax.ShapeDtypeStruct((pops, ws), F32), jax.ShapeDtypeStruct((pops, wf), F32))
    shares, freqs = pl.pallas_call(
        functools.partial(em_kernel, nv, ns),
        out_shape=(pltpu.VMEM((pops, ws), F32), pltpu.VMEM((pops, wf), F32)),
        in_specs=[hbm, hbm, hbm],
        out_specs=(vmem, vmem),
        scratch_shapes=[
            pltpu.VMEM((words, variants), jnp.int32),
            pltpu.VMEM((pops, ws), F32),
            pltpu.VMEM((pops, wf), F32),
            pltpu.VMEM((2, samples, 2 * chunk), F32),
            pltpu.VMEM((nv, pops, ws), F32),
            pltpu.VMEM((ns, PAD, wc), F32),
            pltpu.VMEM((ITERS, chips, pops, 2 * ws), F32),
            pltpu.VMEM((ITERS, PAD, wc), F32),
            pltpu.VMEM((ITERS, 2 * mids, PAD, wc), F32),
            pltpu.VMEM((2, PAD, wc), F32),
            pltpu.VMEM((nv, pops, ws), F32),
            pltpu.VMEM((nv, pops, ws), F32),
            pltpu.VMEM((ITERS, chips, pops, 2 * ws), F32),
            pltpu.VMEM((ITERS, nv, pops, 2 * ws), F32),
            pltpu.VMEM((ITERS, 2, mids, 2 * pops, wc), F32),
            pltpu.VMEM((ITERS, 2, ns, 2 * pops, wc), F32),
            pltpu.VMEM((ns, 2 * pops, wc), F32),
            pltpu.VMEM((PAD, samples), F32),
            pltpu.VMEM((samples, 4 * PAD), BF16),
            pltpu.VMEM((4 * pops, samples), BF16),
            pltpu.VMEM((4 * pops, samples), BF16),
            pltpu.VMEM((2 * PAD, samples), F32),
            dma((3,)),
            dma((nv,)), dma((nv,)),
            dma((ns,)), dma((ns,)),
            dma((ITERS, nv)), dma((ITERS, chips)),
            dma((2,)), dma((2,)),
            dma((ITERS, 2, ns)), dma((ITERS, 2 * mids)),
            dma((nv,)), dma((nv,)),
            dma((ITERS, chips)), dma((ITERS, nv)),
            dma((ITERS, 2, mids)), dma((ITERS, 2, ns)),
            dma((ns,)), dma((ns,)),
        ],
        compiler_params=pltpu.CompilerParams(collective_id=0, has_side_effects=True),
        cost_estimate=pl.CostEstimate(flops=200000000, bytes_accessed=400000, transcendentals=1000000),
    )(dosage, shares_init, freqs_init)
    shares = pltpu.with_memory_space_constraint(shares, pltpu.VMEM)
    freqs = pltpu.with_memory_space_constraint(freqs, pltpu.VMEM)
    return pl.pallas_call(
        hand_out, out_shape=shapes, in_specs=[vmem, vmem], out_specs=(hbm, hbm), scratch_shapes=[dma((2,))],
    )(shares, freqs)


def solution(mesh):
    placed = (P("smp", "var"), P(None, ("smp", "var")), P(None, ("var", "smp")))
    return jax.shard_map(
        functools.partial(body, mesh.shape["var"], mesh.shape["smp"]),
        mesh=mesh,
        in_specs=placed,
        out_specs=(P(None, ("smp", "var")), P(None, ("var", "smp"))),
        check_vma=False,
    )
```

```python
import functools

import jax
import jax.numpy as jnp
from jax import lax
from jax.experimental import pallas as pl
from jax.experimental.pallas import tpu as pltpu
from jax.sharding import PartitionSpec as P

ITERS = 2
CODES = 16
PAD = 16
ROWS = 128
LEVELS = 64
F32 = jnp.float32
BF16 = jnp.bfloat16


def split(x, pieces):
    out = []
    for _ in range(pieces):
        piece = x.astype(BF16)
        out.append(piece)
        x = x - piece.astype(F32)
    return out


def dot(a, b):
    return jnp.dot(a, b, preferred_element_type=F32)


def dot_nt(a, b):
    return lax.dot_general(a, b, (((1,), (1,)), ((), ())), preferred_element_type=F32)


def renewed_shares(old, sums):
    numer = old * sums
    return (numer + 0.5) / (jnp.sum(numer, axis=0, keepdims=True) + 0.5 * old.shape[0])


def renewed_freqs(old, sum_d, sum_b):
    return (old * (sum_d + sum_b) + 0.5) / (old * sum_d + sum_b + 1.0)


def full_rows(x):
    return jnp.concatenate([x, jnp.zeros((PAD - x.shape[0], x.shape[1]), x.dtype)], axis=0)


def em_kernel(
    nv, ns, dosage_hbm, shares_hbm, freqs_hbm, shares_out, freqs_out,
    dosage_ref, shares_ref, freqs_ref, w_ref,
    q_slots, f_slots, p_slots, d_slots, c_slots, e_slots,
    sq_send, sq_recv, sp_send, sp_recv, sc_send, sc_recv, sf_recv,
    q_pad, qt_ref, qd_ref, qb_ref, sq_ref,
    load_sem, q_ss, q_rs, f_ss, f_rs, p_ss, p_rs, d_ss, d_rs, c_ss, c_rs,
    sq_ss, sq_rs, sp_ss, sp_rs, sc_ss, sc_rs, sf_ss, sf_rs,
):
    iv, js = lax.axis_index("var"), lax.axis_index("smp")
    pops, ws = shares_ref.shape
    wf = freqs_ref.shape[1]
    words, variants = dosage_ref.shape
    samples = words * CODES
    half = ns // 2
    mids = half // 2
    chunk = variants // 2
    wc = chunk // mids
    side = js // half
    mesh_ids = pl.DeviceIdType.MESH

    def other_smp(d):
        return lax.rem(js + d, ns)

    def middle(c, i):
        return (1 - c) * half + c * (half - mids) + i

    my_mid_chunk = 1 - side
    my_mid = js - middle(my_mid_chunk, 0)
    place = lax.rem(js, half)
    core, chip, chips = lax.rem(iv, 2), iv // 2, nv // 2
    owner = 2 * chip + 1
    is_owner = core == 1
    central = jnp.logical_and(js >= half - mids, js < half + mids)
    is_mid = jnp.logical_and(is_owner, central)
    first = my_mid_chunk * half + 2 * my_mid
    smp_peers = [other_smp(d) for d in range(1, ns)]
    far_peers = [(1 - side) * (ns - 1 - i) + side * i for i in range(half)]
    near_peers = [side * half + lax.rem(js + d, half) for d in range(half - 1, 0, -1)]
    var_peers = [lax.rem(iv + d, nv) for d in range(1, nv)]

    barrier = pltpu.get_barrier_semaphore()
    for p in far_peers + near_peers:
        pl.semaphore_signal(barrier, inc=1, device_id=(p, iv), device_id_type=mesh_ids)
    for p in var_peers:
        pl.semaphore_signal(barrier, inc=1, device_id=(js, p), device_id_type=mesh_ids)

    load_q = pltpu.make_async_copy(shares_hbm, shares_ref, load_sem.at[0])
    load_f = pltpu.make_async_copy(freqs_hbm, freqs_ref, load_sem.at[1])
    load_d = pltpu.make_async_copy(dosage_hbm, dosage_ref, load_sem.at[2])
    load_q.start()
    load_f.start()
    load_d.start()
    q_pad[...] = jnp.zeros_like(q_pad)
    load_q.wait()
    q_own = shares_ref[...]
    q_own = q_own / jnp.sum(q_own, axis=0, keepdims=True)
    q_slots[iv] = q_own
    load_f.wait()
    f_own = freqs_ref[...]
    beside = jnp.zeros_like(f_own)
    odd = lax.rem(js, 2) == 1
    f_own = jnp.where(odd, jnp.concatenate([beside, f_own], axis=1), jnp.concatenate([f_own, beside], axis=1))
    f_slots[js] = full_rows(f_own)
    pl.semaphore_wait(barrier, ns - 1 + nv - 1)

    def far_copy(src, dst, ss, rs, smp, var):
        return pltpu.make_async_remote_copy(
            src_ref=src, dst_ref=dst, send_sem=ss, recv_sem=rs, device_id=(smp, var), device_id_type=mesh_ids)

    def f_copy(to, slot):
        return far_copy(f_slots.at[slot], f_slots.at[slot], f_ss.at[to], f_rs.at[slot], to, iv)

    def e_copy(slot):
        return far_copy(f_slots.at[first + slot], e_slots.at[slot], d_ss.at[slot], d_rs.at[slot], js, owner)

    def q_copy(to, slot):
        return far_copy(q_slots.at[slot], q_slots.at[slot], q_ss.at[to], q_rs.at[slot], js, to)

    def sq_copy(to, slot):
        return far_copy(sq_send.at[to], sq_recv.at[slot], sq_ss.at[to], sq_rs.at[slot], js, to)

    def sf_copy(c, to, slot):
        return far_copy(
            sc_send.at[ITERS - 1, c, lax.rem(to, half) // 2], sf_recv.at[slot], sf_ss.at[to], sf_rs.at[slot], to, iv)

    def sp_copy(it, j, slot):
        return far_copy(sp_send.at[it, j], sp_recv.at[it, slot], sp_ss.at[it, j], sp_rs.at[it, slot], js, 2 * j + 1)

    def p_copy(it, to, slot):
        return far_copy(p_slots.at[it, slot], p_slots.at[it, slot], p_ss.at[it, to], p_rs.at[it, slot], js, to)

    def sc_copy(it, c, i, g, slot):
        return far_copy(
            sc_send.at[it, c, i], sc_recv.at[it, g, slot], sc_ss.at[it, c, i], sc_rs.at[it, g, slot],
            middle(c, i), owner)

    def c_copy(it, to, slot):
        return far_copy(c_slots.at[it, slot], c_slots.at[it, slot], c_ss.at[it, 1, to], c_rs.at[it, slot], to, iv)

    def d_copy(it, to, slot):
        return far_copy(d_slots.at[it], c_slots.at[it, slot], c_ss.at[it, 0, to], c_rs.at[it, slot], to, iv - 1)

    sent = []

    def start(copy, when=None):
        sent.append((copy, when))
        if when is None:
            copy.start()
        else:
            pl.when(when)(copy.start)

    for p in far_peers + near_peers:
        start(f_copy(p, js))
    for p in var_peers:
        start(q_copy(p, iv))

    load_d.wait()
    blocks = samples // ROWS
    ones = jnp.ones((8, chunk), BF16)
    shape3 = (ROWS // CODES, CODES, chunk)
    shifts = 2 * lax.broadcasted_iota(jnp.int32, shape3, 1)
    level = 16 * lax.broadcasted_iota(jnp.int32, shape3, 0) + lax.broadcasted_iota(jnp.int32, shape3, 1)
    level = jnp.bitwise_and(19 * level + 27 * lax.broadcasted_iota(jnp.int32, shape3, 2), LEVELS - 1)
    step = (level.astype(F32) - 0.5 * (LEVELS - 1)) * (2.0 ** -7 / LEVELS) + 1.0
    counts = []
    for b in range(blocks):
        here = slice(b * ROWS, (b + 1) * ROWS)
        count = jnp.zeros((8, ROWS), F32)
        for c in range(2):
            packed = dosage_ref[b * ROWS // CODES:(b + 1) * ROWS // CODES, c * chunk:(c + 1) * chunk]
            codes = jnp.bitwise_and(jnp.right_shift(jnp.broadcast_to(packed[:, None, :], shape3), shifts), 3)
            live = codes < 3
            alt = jnp.where(live, codes.astype(F32), 0.0)
            both = jnp.where(live, 2.0, 0.0)
            w_ref[c, here, 0:chunk] = (alt * step).reshape(ROWS, chunk)
            w_ref[c, here, chunk:2 * chunk] = ((both - alt) * step).reshape(ROWS, chunk)
            count = count + dot_nt(ones, both.reshape(ROWS, chunk).astype(BF16))
        counts.append(count[0:1])
    counts = jnp.concatenate(counts, axis=1)

    for it in range(ITERS):
        last = it + 1 == ITERS

        if it == 0:
            for p in var_peers:
                q_copy(p, p).wait_recv()
            for v in range(nv):
                q_pad[0:pops, v * ws:(v + 1) * ws] = q_slots[v]
        else:
            for j in range(chips):
                pl.when(iv != 2 * j + 1)(p_copy(it, iv, j).wait_recv)
            for j in range(chips):
                q_pad[0:pops, 2 * j * ws:2 * (j + 1) * ws] = p_slots[it, j]
        qh, qm = split(q_pad[...], 2)
        qs = jnp.concatenate([qh, qm, qh, qm], axis=0)
        qt_ref[...] = qs.astype(F32).T.astype(BF16)
        qh, qm = qh.astype(F32)[0:pops], qm.astype(F32)[0:pops]
        none = jnp.zeros_like(qh)
        qd_ref[...] = jnp.concatenate([qh, none, qm, none], axis=0).astype(BF16)
        qb_ref[...] = jnp.concatenate([none, qh, none, qm], axis=0).astype(BF16)

        for t in range(2):
            c = side if (it == 0) == (t == 0) else 1 - side
            if it == 0:
                for i in range(half):
                    p = c * half + lax.rem(js + i, half)
                    if t or i:
                        f_copy(p, p).wait_recv()
                for i in range(2 * t):
                    start(e_copy(i), jnp.logical_and(central, core == 0))
                f_all = [f_slots[c * half + 2 * i] + f_slots[c * half + 2 * i + 1] for i in range(mids)]
            else:
                for i in range(mids):
                    slot = c * mids + i
                    copy = c_copy(it, js, slot)
                    pl.when(jnp.logical_or(core == 0, middle(c, i) != js))(copy.wait_recv)
                f_all = [c_slots[it, c * mids + i] for i in range(mids)]
            fh, fm = split(jnp.concatenate(f_all, axis=1), 2)
            fs = jnp.concatenate([fh, fh, fm, fm], axis=0)
            fg = jnp.concatenate([fh, fm], axis=0)

            kept = []
            sums = jnp.zeros((4 * pops, chunk), F32)
            for b in range(blocks):
                here = slice(b * ROWS, (b + 1) * ROWS)
                probs = dot(qt_ref[here, :], fs)
                bb = w_ref[c, here, chunk:2 * chunk] * (1.0 / (1.0 - probs))
                dd = w_ref[c, here, 0:chunk] * (1.0 / probs) - bb
                dh, bh = dd.astype(BF16), bb.astype(BF16)
                sums = sums + (dot(qd_ref[:, here], dh) + dot(qb_ref[:, here], bh))
                kept.append(dh)
            sums = sums[0:2 * pops] + sums[2 * pops:4 * pops]
            for i in range(mids):
                sc_send[it, c, i] = sums[:, i * wc:(i + 1) * wc]
            if last:
                for p in far_peers if t == 0 else near_peers:
                    start(sf_copy(c, p, js))
            else:
                for i in range(mids):
                    start(sc_copy(it, c, i, core, js), jnp.logical_or(core == 0, middle(c, i) != js))
            if t == 0:
                sq_ref[...] = jnp.concatenate([dot_nt(fg, x) for x in kept], axis=1)

        sum_q = sq_ref[...] + jnp.concatenate([dot_nt(fg, x) for x in kept], axis=1)
        sum_q = sum_q[0:PAD] + sum_q[PAD:2 * PAD]
        sum_q = sum_q + (counts - jnp.sum(q_pad[...] * sum_q, axis=0, keepdims=True))
        sum_q = sum_q[0:pops]
        if not last:
            for j in range(chips):
                sp_send[it, j] = sum_q[:, 2 * j * ws:2 * (j + 1) * ws]
            for j in range(chips):
                start(sp_copy(it, j, iv), iv != 2 * j + 1)

            @pl.when(is_owner)
            def _():
                total = sp_send[it, chip]
                for p in var_peers:
                    sp_copy(it, chip, p).wait_recv()
                    total = total + sp_recv[it, p]
                if it == 0:
                    q_old = jnp.concatenate([q_slots[2 * chip], q_slots[2 * chip + 1]], axis=1)
                else:
                    q_old = p_slots[it, chip]
                p_slots[it + 1, chip] = renewed_shares(q_old, total)

            for p in var_peers:
                start(p_copy(it + 1, p, chip), is_owner)

            slot = my_mid_chunk * mids + my_mid
            for g in (1, 0):

                @pl.when(is_mid)
                def _():
                    if g:
                        total = sc_send[it, my_mid_chunk, my_mid]
                        peers = smp_peers
                    else:
                        total = jnp.zeros((2 * pops, wc), F32)
                        peers = smp_peers + [js]
                    for p in peers:
                        sc_copy(it, my_mid_chunk, my_mid, g, p).wait_recv()
                        total = total + sc_recv[it, g, p]
                    if it == 0 and g:
                        f_old = f_slots[first] + f_slots[first + 1]
                    elif it == 0:
                        e_copy(0).wait_recv()
                        e_copy(1).wait_recv()
                        f_old = e_slots[0] + e_slots[1]
                    else:
                        f_old = c_slots[it, slot] if g else d_slots[it]
                    new = full_rows(renewed_freqs(f_old[0:pops], total[0:pops], total[pops:2 * pops]))
                    if g:
                        c_slots[it + 1, slot] = new
                    else:
                        d_slots[it + 1] = new

                for p in far_peers + near_peers + ([] if g else [js]):
                    start((c_copy if g else d_copy)(it + 1, p, slot), is_mid)
        else:
            for v in range(nv):
                sq_send[v] = sum_q[:, v * ws:(v + 1) * ws]
            for p in var_peers:
                start(sq_copy(p, iv))
            total = sq_send[iv]
            for p in var_peers:
                sq_copy(p, p).wait_recv()
                total = total + sq_recv[p]
            pair = p_slots[it, chip]
            shares_out[...] = renewed_shares(jnp.where(core == 0, pair[:, 0:ws], pair[:, ws:2 * ws]), total)

            for copy, when in sent:
                if when is None:
                    copy.wait_send()
                else:
                    pl.when(when)(copy.wait_send)

            total = sc_send[it, side, place // 2]
            for p in smp_peers:
                sf_copy(side, p, p).wait_recv()
                total = total + sf_recv[p]
            pair = renewed_freqs(c_slots[it, side * mids + place // 2][0:pops], total[0:pops], total[pops:2 * pops])
            freqs_out[...] = jnp.where(odd, pair[:, wf:2 * wf], pair[:, 0:wf])


def hand_out(shares_ref, freqs_ref, shares_out, freqs_out, sems):
    copies = [
        pltpu.make_async_copy(shares_ref, shares_out, sems.at[0]),
        pltpu.make_async_copy(freqs_ref, freqs_out, sems.at[1]),
    ]
    for copy in copies:
        copy.start()
    for copy in copies:
        copy.wait()


def body(nv, ns, dosage, shares_init, freqs_init):
    pops, ws = shares_init.shape
    wf = freqs_init.shape[1]
    words, variants = dosage.shape
    samples = words * CODES
    chunk = variants // 2
    mids = ns // 4
    chips = nv // 2
    wc = chunk // mids
    vmem = pl.BlockSpec(memory_space=pltpu.VMEM)
    hbm = pl.BlockSpec(memory_space=pl.ANY)
    dma = pltpu.SemaphoreType.DMA
    shapes = (jax.ShapeDtypeStruct((pops, ws), F32), jax.ShapeDtypeStruct((pops, wf), F32))
    shares, freqs = pl.pallas_call(
        functools.partial(em_kernel, nv, ns),
        out_shape=(pltpu.VMEM((pops, ws), F32), pltpu.VMEM((pops, wf), F32)),
        in_specs=[hbm, hbm, hbm],
        out_specs=(vmem, vmem),
        scratch_shapes=[
            pltpu.VMEM((words, variants), jnp.int32),
            pltpu.VMEM((pops, ws), F32),
            pltpu.VMEM((pops, wf), F32),
            pltpu.VMEM((2, samples, 2 * chunk), F32),
            pltpu.VMEM((nv, pops, ws), F32),
            pltpu.VMEM((ns, PAD, wc), F32),
            pltpu.VMEM((ITERS, chips, pops, 2 * ws), F32),
            pltpu.VMEM((ITERS, PAD, wc), F32),
            pltpu.VMEM((ITERS, 2 * mids, PAD, wc), F32),
            pltpu.VMEM((2, PAD, wc), F32),
            pltpu.VMEM((nv, pops, ws), F32),
            pltpu.VMEM((nv, pops, ws), F32),
            pltpu.VMEM((ITERS, chips, pops, 2 * ws), F32),
            pltpu.VMEM((ITERS, nv, pops, 2 * ws), F32),
            pltpu.VMEM((ITERS, 2, mids, 2 * pops, wc), F32),
            pltpu.VMEM((ITERS, 2, ns, 2 * pops, wc), F32),
            pltpu.VMEM((ns, 2 * pops, wc), F32),
            pltpu.VMEM((PAD, samples), F32),
            pltpu.VMEM((samples, 4 * PAD), BF16),
            pltpu.VMEM((4 * pops, samples), BF16),
            pltpu.VMEM((4 * pops, samples), BF16),
            pltpu.VMEM((2 * PAD, samples), F32),
            dma((3,)),
            dma((nv,)), dma((nv,)),
            dma((ns,)), dma((ns,)),
            dma((ITERS, nv)), dma((ITERS, chips)),
            dma((2,)), dma((2,)),
            dma((ITERS, 2, ns)), dma((ITERS, 2 * mids)),
            dma((nv,)), dma((nv,)),
            dma((ITERS, chips)), dma((ITERS, nv)),
            dma((ITERS, 2, mids)), dma((ITERS, 2, ns)),
            dma((ns,)), dma((ns,)),
        ],
        compiler_params=pltpu.CompilerParams(collective_id=0, has_side_effects=True),
        cost_estimate=pl.CostEstimate(flops=200000000, bytes_accessed=400000, transcendentals=1000000),
    )(dosage, shares_init, freqs_init)
    shares = pltpu.with_memory_space_constraint(shares, pltpu.VMEM)
    freqs = pltpu.with_memory_space_constraint(freqs, pltpu.VMEM)
    return pl.pallas_call(
        hand_out, out_shape=shapes, in_specs=[vmem, vmem], out_specs=(hbm, hbm), scratch_shapes=[dma((2,))],
    )(shares, freqs)


def solution(mesh):
    placed = (P("smp", "var"), P(None, ("smp", "var")), P(None, ("var", "smp")))
    return jax.shard_map(
        functools.partial(body, mesh.shape["var"], mesh.shape["smp"]),
        mesh=mesh,
        in_specs=placed,
        out_specs=(P(None, ("smp", "var")), P(None, ("var", "smp"))),
        check_vma=False,
    )
```

```python
import functools

import jax
import jax.numpy as jnp
from jax import lax
from jax.experimental import pallas as pl
from jax.experimental.pallas import tpu as pltpu
from jax.sharding import PartitionSpec as P

ITERS = 2
CODES = 16
PAD = 16
ROWS = 128
LEVELS = 64
F32 = jnp.float32
BF16 = jnp.bfloat16


def split(x, pieces):
    out = []
    for _ in range(pieces):
        piece = x.astype(BF16)
        out.append(piece)
        x = x - piece.astype(F32)
    return out


def dot(a, b):
    return jnp.dot(a, b, preferred_element_type=F32)


def dot_nt(a, b):
    return lax.dot_general(a, b, (((1,), (1,)), ((), ())), preferred_element_type=F32)


def renewed_shares(old, sums):
    numer = old * sums
    return (numer + 0.5) / (jnp.sum(numer, axis=0, keepdims=True) + 0.5 * old.shape[0])


def renewed_freqs(old, sum_d, sum_b):
    return (old * (sum_d + sum_b) + 0.5) / (old * sum_d + sum_b + 1.0)


def full_rows(x):
    return jnp.concatenate([x, jnp.zeros((PAD - x.shape[0], x.shape[1]), x.dtype)], axis=0)


def em_kernel(
    nv, ns, dosage_hbm, shares_hbm, freqs_hbm, shares_out, freqs_out,
    dosage_ref, shares_ref, freqs_ref, w_ref,
    q_slots, f_slots, p_slots, d_slots, c_slots, e_slots,
    sq_send, sq_recv, sp_send, sp_recv, sc_send, sc_recv, sf_recv,
    q_pad, qt_ref, qd_ref, qb_ref, sq_ref,
    load_sem, q_ss, q_rs, f_ss, f_rs, p_ss, p_rs, d_ss, d_rs, c_ss, c_rs,
    sq_ss, sq_rs, sp_ss, sp_rs, sc_ss, sc_rs, sf_ss, sf_rs,
):
    iv, js = lax.axis_index("var"), lax.axis_index("smp")
    pops, ws = shares_ref.shape
    wf = freqs_ref.shape[1]
    words, variants = dosage_ref.shape
    samples = words * CODES
    half = ns // 2
    mids = half // 2
    chunk = variants // 2
    wc = chunk // mids
    side = js // half
    mesh_ids = pl.DeviceIdType.MESH

    def other_smp(d):
        return lax.rem(js + d, ns)

    def middle(c, i):
        return (1 - c) * half + c * (half - mids) + i

    my_mid_chunk = 1 - side
    my_mid = js - middle(my_mid_chunk, 0)
    place = lax.rem(js, half)
    core, chip, chips = lax.rem(iv, 2), iv // 2, nv // 2
    owner = 2 * chip + 1
    is_owner = core == 1
    central = jnp.logical_and(js >= half - mids, js < half + mids)
    is_mid = jnp.logical_and(is_owner, central)
    first = my_mid_chunk * half + 2 * my_mid
    smp_peers = [other_smp(d) for d in range(1, ns)]
    far_peers = [(1 - side) * (ns - 1 - i) + side * i for i in range(half)]
    near_peers = [side * half + lax.rem(js + d, half) for d in range(half - 1, 0, -1)]
    var_peers = [lax.rem(iv + d, nv) for d in range(1, nv)]

    barrier = pltpu.get_barrier_semaphore()
    for p in far_peers + near_peers:
        pl.semaphore_signal(barrier, inc=1, device_id=(p, iv), device_id_type=mesh_ids)
    for p in var_peers:
        pl.semaphore_signal(barrier, inc=1, device_id=(js, p), device_id_type=mesh_ids)

    load_q = pltpu.make_async_copy(shares_hbm, shares_ref, load_sem.at[0])
    load_f = pltpu.make_async_copy(freqs_hbm, freqs_ref, load_sem.at[1])
    load_d = pltpu.make_async_copy(dosage_hbm, dosage_ref, load_sem.at[2])
    load_q.start()
    load_f.start()
    load_d.start()
    q_pad[...] = jnp.zeros_like(q_pad)
    load_q.wait()
    q_own = shares_ref[...]
    q_own = q_own / jnp.sum(q_own, axis=0, keepdims=True)
    q_slots[iv] = q_own
    load_f.wait()
    f_own = freqs_ref[...]
    beside = jnp.zeros_like(f_own)
    odd = lax.rem(js, 2) == 1
    f_own = jnp.where(odd, jnp.concatenate([beside, f_own], axis=1), jnp.concatenate([f_own, beside], axis=1))
    f_slots[js] = full_rows(f_own)
    pl.semaphore_wait(barrier, ns - 1 + nv - 1)

    def far_copy(src, dst, ss, rs, smp, var):
        return pltpu.make_async_remote_copy(
            src_ref=src, dst_ref=dst, send_sem=ss, recv_sem=rs, device_id=(smp, var), device_id_type=mesh_ids)

    def f_copy(to, slot):
        return far_copy(f_slots.at[slot], f_slots.at[slot], f_ss.at[to], f_rs.at[slot], to, iv)

    def e_copy(slot):
        return far_copy(f_slots.at[first + slot], e_slots.at[slot], d_ss.at[slot], d_rs.at[slot], js, owner)

    def q_copy(to, slot):
        return far_copy(q_slots.at[slot], q_slots.at[slot], q_ss.at[to], q_rs.at[slot], js, to)

    def sq_copy(to, slot):
        return far_copy(sq_send.at[to], sq_recv.at[slot], sq_ss.at[to], sq_rs.at[slot], js, to)

    def sf_copy(c, to, slot):
        return far_copy(
            sc_send.at[ITERS - 1, c, lax.rem(to, half) // 2], sf_recv.at[slot], sf_ss.at[to], sf_rs.at[slot], to, iv)

    def sp_copy(it, j, slot):
        return far_copy(sp_send.at[it, j], sp_recv.at[it, slot], sp_ss.at[it, j], sp_rs.at[it, slot], js, 2 * j + 1)

    def p_copy(it, to, slot):
        return far_copy(p_slots.at[it, slot], p_slots.at[it, slot], p_ss.at[it, to], p_rs.at[it, slot], js, to)

    def sc_copy(it, c, i, g, slot):
        return far_copy(
            sc_send.at[it, c, i], sc_recv.at[it, g, slot], sc_ss.at[it, c, i], sc_rs.at[it, g, slot],
            middle(c, i), owner)

    def c_copy(it, to, slot):
        return far_copy(c_slots.at[it, slot], c_slots.at[it, slot], c_ss.at[it, 1, to], c_rs.at[it, slot], to, iv)

    def d_copy(it, to, slot):
        return far_copy(d_slots.at[it], c_slots.at[it, slot], c_ss.at[it, 0, to], c_rs.at[it, slot], to, iv - 1)

    sent = []

    def start(copy, when=None):
        sent.append((copy, when))
        if when is None:
            copy.start()
        else:
            pl.when(when)(copy.start)

    for p in far_peers:
        start(f_copy(p, js))
    for p in var_peers:
        start(q_copy(p, iv))
    for p in near_peers:
        start(f_copy(p, js))

    load_d.wait()
    blocks = samples // ROWS
    ones = jnp.ones((8, chunk), BF16)
    shape3 = (ROWS // CODES, CODES, chunk)
    shifts = 2 * lax.broadcasted_iota(jnp.int32, shape3, 1)
    level = 16 * lax.broadcasted_iota(jnp.int32, shape3, 0) + lax.broadcasted_iota(jnp.int32, shape3, 1)
    level = jnp.bitwise_and(19 * level + 27 * lax.broadcasted_iota(jnp.int32, shape3, 2), LEVELS - 1)
    step = (level.astype(F32) - 0.5 * (LEVELS - 1)) * (2.0 ** -7 / LEVELS) + 1.0
    counts = []
    for b in range(blocks):
        here = slice(b * ROWS, (b + 1) * ROWS)
        count = jnp.zeros((8, ROWS), F32)
        for c in range(2):
            packed = dosage_ref[b * ROWS // CODES:(b + 1) * ROWS // CODES, c * chunk:(c + 1) * chunk]
            codes = jnp.bitwise_and(jnp.right_shift(jnp.broadcast_to(packed[:, None, :], shape3), shifts), 3)
            live = codes < 3
            alt = jnp.where(live, codes.astype(F32), 0.0)
            both = jnp.where(live, 2.0, 0.0)
            w_ref[c, here, 0:chunk] = (alt * step).reshape(ROWS, chunk)
            w_ref[c, here, chunk:2 * chunk] = ((both - alt) * step).reshape(ROWS, chunk)
            count = count + dot_nt(ones, both.reshape(ROWS, chunk).astype(BF16))
        counts.append(count[0:1])
    counts = jnp.concatenate(counts, axis=1)

    for it in range(ITERS):
        last = it + 1 == ITERS

        if it == 0:
            for p in var_peers:
                q_copy(p, p).wait_recv()
            for v in range(nv):
                q_pad[0:pops, v * ws:(v + 1) * ws] = q_slots[v]
        else:
            for j in range(chips):
                pl.when(iv != 2 * j + 1)(p_copy(it, iv, j).wait_recv)
            for j in range(chips):
                q_pad[0:pops, 2 * j * ws:2 * (j + 1) * ws] = p_slots[it, j]
        qh, qm = split(q_pad[...], 2)
        qs = jnp.concatenate([qh, qm, qh, qm], axis=0)
        qt_ref[...] = qs.astype(F32).T.astype(BF16)
        qh, qm = qh.astype(F32)[0:pops], qm.astype(F32)[0:pops]
        none = jnp.zeros_like(qh)
        qd_ref[...] = jnp.concatenate([qh, none, qm, none], axis=0).astype(BF16)
        qb_ref[...] = jnp.concatenate([none, qh, none, qm], axis=0).astype(BF16)

        for t in range(2):
            c = side if (it == 0) == (t == 0) else 1 - side
            if it == 0:
                for i in range(half):
                    p = c * half + lax.rem(js + i, half)
                    if t or i:
                        f_copy(p, p).wait_recv()
                for i in range(2 * t):
                    start(e_copy(i), jnp.logical_and(central, core == 0))
                f_all = [f_slots[c * half + 2 * i] + f_slots[c * half + 2 * i + 1] for i in range(mids)]
            else:
                for i in range(mids):
                    slot = c * mids + i
                    copy = c_copy(it, js, slot)
                    pl.when(jnp.logical_or(core == 0, middle(c, i) != js))(copy.wait_recv)
                f_all = [c_slots[it, c * mids + i] for i in range(mids)]
            fh, fm = split(jnp.concatenate(f_all, axis=1), 2)
            fs = jnp.concatenate([fh, fh, fm, fm], axis=0)
            fg = jnp.concatenate([fh, fm], axis=0)

            kept = []
            sums = jnp.zeros((4 * pops, chunk), F32)
            for b in range(blocks):
                here = slice(b * ROWS, (b + 1) * ROWS)
                probs = dot(qt_ref[here, :], fs)
                bb = w_ref[c, here, chunk:2 * chunk] * (1.0 / (1.0 - probs))
                dd = w_ref[c, here, 0:chunk] * (1.0 / probs) - bb
                dh, bh = dd.astype(BF16), bb.astype(BF16)
                sums = sums + (dot(qd_ref[:, here], dh) + dot(qb_ref[:, here], bh))
                kept.append(dh)
            sums = sums[0:2 * pops] + sums[2 * pops:4 * pops]
            for i in range(mids):
                sc_send[it, c, i] = sums[:, i * wc:(i + 1) * wc]
            if last:
                for p in far_peers if t == 0 else near_peers:
                    start(sf_copy(c, p, js))
            else:
                for i in range(mids):
                    start(sc_copy(it, c, i, core, js), jnp.logical_or(core == 0, middle(c, i) != js))
            if t == 0:
                sq_ref[...] = dot_nt(fg, jnp.concatenate(kept, axis=0))

        sum_q = sq_ref[...] + dot_nt(fg, jnp.concatenate(kept, axis=0))
        sum_q = sum_q[0:PAD] + sum_q[PAD:2 * PAD]
        sum_q = sum_q + (counts - jnp.sum(q_pad[...] * sum_q, axis=0, keepdims=True))
        sum_q = sum_q[0:pops]
        if not last:
            for j in range(chips):
                sp_send[it, j] = sum_q[:, 2 * j * ws:2 * (j + 1) * ws]
            for j in range(chips):
                start(sp_copy(it, j, iv), iv != 2 * j + 1)

            @pl.when(is_owner)
            def _():
                total = sp_send[it, chip]
                for p in var_peers:
                    sp_copy(it, chip, p).wait_recv()
                    total = total + sp_recv[it, p]
                if it == 0:
                    q_old = jnp.concatenate([q_slots[2 * chip], q_slots[2 * chip + 1]], axis=1)
                else:
                    q_old = p_slots[it, chip]
                p_slots[it + 1, chip] = renewed_shares(q_old, total)

            for p in var_peers:
                start(p_copy(it + 1, p, chip), is_owner)

            slot = my_mid_chunk * mids + my_mid
            for g in (1, 0):

                @pl.when(is_mid)
                def _():
                    if g:
                        total = sc_send[it, my_mid_chunk, my_mid]
                        peers = smp_peers
                    else:
                        total = jnp.zeros((2 * pops, wc), F32)
                        peers = smp_peers + [js]
                    for p in peers:
                        sc_copy(it, my_mid_chunk, my_mid, g, p).wait_recv()
                        total = total + sc_recv[it, g, p]
                    if it == 0 and g:
                        f_old = f_slots[first] + f_slots[first + 1]
                    elif it == 0:
                        e_copy(0).wait_recv()
                        e_copy(1).wait_recv()
                        f_old = e_slots[0] + e_slots[1]
                    else:
                        f_old = c_slots[it, slot] if g else d_slots[it]
                    new = full_rows(renewed_freqs(f_old[0:pops], total[0:pops], total[pops:2 * pops]))
                    if g:
                        c_slots[it + 1, slot] = new
                    else:
                        d_slots[it + 1] = new

                for p in far_peers + near_peers + ([] if g else [js]):
                    start((c_copy if g else d_copy)(it + 1, p, slot), is_mid)
        else:
            for v in range(nv):
                sq_send[v] = sum_q[:, v * ws:(v + 1) * ws]
            for p in var_peers:
                start(sq_copy(p, iv))
            total = sq_send[iv]
            for p in var_peers:
                sq_copy(p, p).wait_recv()
                total = total + sq_recv[p]
            pair = p_slots[it, chip]
            shares_out[...] = renewed_shares(jnp.where(core == 0, pair[:, 0:ws], pair[:, ws:2 * ws]), total)

            for copy, when in sent:
                if when is None:
                    copy.wait_send()
                else:
                    pl.when(when)(copy.wait_send)

            total = sc_send[it, side, place // 2]
            for p in smp_peers:
                sf_copy(side, p, p).wait_recv()
                total = total + sf_recv[p]
            pair = renewed_freqs(c_slots[it, side * mids + place // 2][0:pops], total[0:pops], total[pops:2 * pops])
            freqs_out[...] = jnp.where(odd, pair[:, wf:2 * wf], pair[:, 0:wf])


def hand_out(shares_ref, freqs_ref, shares_out, freqs_out, sems):
    copies = [
        pltpu.make_async_copy(shares_ref, shares_out, sems.at[0]),
        pltpu.make_async_copy(freqs_ref, freqs_out, sems.at[1]),
    ]
    for copy in copies:
        copy.start()
    for copy in copies:
        copy.wait()


def body(nv, ns, dosage, shares_init, freqs_init):
    pops, ws = shares_init.shape
    wf = freqs_init.shape[1]
    words, variants = dosage.shape
    samples = words * CODES
    chunk = variants // 2
    mids = ns // 4
    chips = nv // 2
    wc = chunk // mids
    vmem = pl.BlockSpec(memory_space=pltpu.VMEM)
    hbm = pl.BlockSpec(memory_space=pl.ANY)
    dma = pltpu.SemaphoreType.DMA
    shapes = (jax.ShapeDtypeStruct((pops, ws), F32), jax.ShapeDtypeStruct((pops, wf), F32))
    shares, freqs = pl.pallas_call(
        functools.partial(em_kernel, nv, ns),
        out_shape=(pltpu.VMEM((pops, ws), F32), pltpu.VMEM((pops, wf), F32)),
        in_specs=[hbm, hbm, hbm],
        out_specs=(vmem, vmem),
        scratch_shapes=[
            pltpu.VMEM((words, variants), jnp.int32),
            pltpu.VMEM((pops, ws), F32),
            pltpu.VMEM((pops, wf), F32),
            pltpu.VMEM((2, samples, 2 * chunk), F32),
            pltpu.VMEM((nv, pops, ws), F32),
            pltpu.VMEM((ns, PAD, wc), F32),
            pltpu.VMEM((ITERS, chips, pops, 2 * ws), F32),
            pltpu.VMEM((ITERS, PAD, wc), F32),
            pltpu.VMEM((ITERS, 2 * mids, PAD, wc), F32),
            pltpu.VMEM((2, PAD, wc), F32),
            pltpu.VMEM((nv, pops, ws), F32),
            pltpu.VMEM((nv, pops, ws), F32),
            pltpu.VMEM((ITERS, chips, pops, 2 * ws), F32),
            pltpu.VMEM((ITERS, nv, pops, 2 * ws), F32),
            pltpu.VMEM((ITERS, 2, mids, 2 * pops, wc), F32),
            pltpu.VMEM((ITERS, 2, ns, 2 * pops, wc), F32),
            pltpu.VMEM((ns, 2 * pops, wc), F32),
            pltpu.VMEM((PAD, samples), F32),
            pltpu.VMEM((samples, 4 * PAD), BF16),
            pltpu.VMEM((4 * pops, samples), BF16),
            pltpu.VMEM((4 * pops, samples), BF16),
            pltpu.VMEM((2 * PAD, samples), F32),
            dma((3,)),
            dma((nv,)), dma((nv,)),
            dma((ns,)), dma((ns,)),
            dma((ITERS, nv)), dma((ITERS, chips)),
            dma((2,)), dma((2,)),
            dma((ITERS, 2, ns)), dma((ITERS, 2 * mids)),
            dma((nv,)), dma((nv,)),
            dma((ITERS, chips)), dma((ITERS, nv)),
            dma((ITERS, 2, mids)), dma((ITERS, 2, ns)),
            dma((ns,)), dma((ns,)),
        ],
        compiler_params=pltpu.CompilerParams(collective_id=0, has_side_effects=True),
        cost_estimate=pl.CostEstimate(flops=200000000, bytes_accessed=400000, transcendentals=1000000),
    )(dosage, shares_init, freqs_init)
    shares = pltpu.with_memory_space_constraint(shares, pltpu.VMEM)
    freqs = pltpu.with_memory_space_constraint(freqs, pltpu.VMEM)
    return pl.pallas_call(
        hand_out, out_shape=shapes, in_specs=[vmem, vmem], out_specs=(hbm, hbm), scratch_shapes=[dma((2,))],
    )(shares, freqs)


def solution(mesh):
    placed = (P("smp", "var"), P(None, ("smp", "var")), P(None, ("var", "smp")))
    return jax.shard_map(
        functools.partial(body, mesh.shape["var"], mesh.shape["smp"]),
        mesh=mesh,
        in_specs=placed,
        out_specs=(P(None, ("smp", "var")), P(None, ("var", "smp"))),
        check_vma=False,
    )
```
